32 devices in a mesh: seq: 8 (over z, y), tp: 4 (over x, core).
Axes of the slice: x: 2, y: 2, z: 4, core: 2. Of those that a mesh axis runs over, the one named last changes fastest.
Arguments:
- tokens: bfloat16 [8192, 1024], P(('seq', 'tp')), may hold values from -6 to 6
- fine_gain: float32 [1024], replicated, may hold values from 0.1 to 1.9
- fine_query: bfloat16 [1024, 1024], replicated, may hold values from -2.0625 to 2.0625
- fine_keyval: bfloat16 [1024, 2048], replicated, may hold values from -0.125 to 0.125
- fine_out: bfloat16 [1024, 1024], replicated, may hold values from -0.1875 to 0.1875
- down_weight: bfloat16 [1024, 4096], P(None, 'tp'), may hold values from -0.1875 to 0.1875
- coarse_gain: float32 [4096], replicated, may hold values from 0.1 to 1.9
- coarse_query: bfloat16 [4096, 4096], P('seq', 'tp'), may hold values from -1.03125 to 1.03125
- coarse_keyval: bfloat16 [4096, 2, 4096], P('seq', None, 'tp'), may hold values from -0.0625 to 0.0625
- coarse_out: bfloat16 [4096, 4096], P('tp'), may hold values from -0.09375 to 0.09375
- up_weight: bfloat16 [4096, 1024], P('tp'), may hold values from -0.09375 to 0.09375
Outputs:
- result: bfloat16 [8192, 1024], P(('seq', 'tp'))
The draws below stay inside these ranges and needn't reach their ends.
All inputs are finite; a program needn't handle non-finite values.
Results may differ from the reference program's by a relative error of at most 0.02.
Values may be sent and summed in bfloat16 or wider, within the bound.
A program may use at most 192 MiB of HBM per device.

```python
import math
import jax
import jax.numpy as jnp
from jax import lax

D_FINE = 1024
D_COARSE = 4096
HEAD = 128
WINDOW = 256
SHORT = 8
TOKENS = 8192


def paired_weights(key, marker, rows, cols, spread):
    base = jax.random.fold_in(key, marker)
    first, second, third = jax.random.split(base, 3)
    root = jnp.sqrt(jnp.float32(rows))
    key_part = jax.random.truncated_normal(first, -4.0, 4.0, (rows, cols), jnp.float32) / root
    value_part = jax.random.truncated_normal(second, -4.0, 4.0, (rows, cols), jnp.float32) / root
    query_part = jax.random.truncated_normal(third, -4.0, 4.0, (rows, cols), jnp.float32) / root
    query_part = spread * query_part
    return (query_part, key_part, value_part)


def draw_fine_query(key, part):
    return paired_weights(key, 11, D_FINE, D_FINE, 1.0)[0].astype(jnp.bfloat16)


def draw_fine_keyval(key, part):
    drawn = paired_weights(key, 11, D_FINE, D_FINE, 1.0)
    return jnp.concatenate([drawn[1], drawn[2]], 1).astype(jnp.bfloat16)


def draw_coarse_query(key, part):
    return paired_weights(key, 23, D_COARSE, D_COARSE, 3.0)[0].astype(jnp.bfloat16)


def draw_coarse_keyval(key, part):
    drawn = paired_weights(key, 23, D_COARSE, D_COARSE, 3.0)
    return jnp.stack([drawn[1], drawn[2]], 1).astype(jnp.bfloat16)


def level_of(key, extent, cuts, smallest, high):
    gain, own = 1.0, jax.random.fold_in(key, 6)
    for dim, parts in cuts:
        draws = jnp.exp(jax.random.uniform(jax.random.fold_in(own, dim), (parts,), jnp.float32, smallest / len(cuts), high / len(cuts)))
        gain = gain * jnp.repeat(draws, extent[dim] // parts).reshape([-1 if axis == dim else 1 for axis in range(len(extent))])
    return gain


def noise(rng, dims, deviation, bound, cuts=(), kind=jnp.bfloat16):
    factor_of = level_of(rng, dims, cuts, -0.22, 0.18) if cuts else 1.0
    values = jax.random.normal(rng, dims, jnp.float32) * deviation * factor_of
    return jnp.minimum(jnp.maximum(values, -bound), bound).astype(kind)


def setup_inputs(seed: int = 0) -> dict:
    key_list = jax.random.split(jax.random.key(seed), 12)
    tokens = noise(key_list[0], (TOKENS, D_FINE), 1.0, 6.0, ((0, 32),))
    fine_gain = jnp.clip(1.0 + 0.18 * jax.random.normal(key_list[1], (D_FINE,), jnp.float32), 0.1, 1.9)
    fine_query = draw_fine_query(jax.random.fold_in(key_list[11], 71), 0)
    fine_keyval = draw_fine_keyval(jax.random.fold_in(key_list[11], 71), 0)
    fine_out = noise(key_list[4], (D_FINE, D_FINE), D_FINE ** -0.5, 0.1875)
    down_weight = noise(key_list[5], (D_FINE, D_COARSE), D_FINE ** -0.5, 0.1875, ((1, 4),))
    coarse_gain = jnp.clip(1.0 + 0.18 * jax.random.normal(key_list[6], (D_COARSE,), jnp.float32), 0.1, 1.9)
    coarse_query = draw_coarse_query(jax.random.fold_in(key_list[11], 71), 0)
    coarse_keyval = draw_coarse_keyval(jax.random.fold_in(key_list[11], 71), 0)
    coarse_out = noise(key_list[9], (D_COARSE, D_COARSE), D_COARSE ** -0.5, 0.09375, ((0, 4),))
    up_weight = noise(key_list[10], (D_COARSE, D_FINE), D_COARSE ** -0.5, 0.09375, ((0, 4),))
    return dict(tokens=tokens, fine_gain=fine_gain, fine_query=fine_query, fine_keyval=fine_keyval, fine_out=fine_out, down_weight=down_weight, coarse_gain=coarse_gain, coarse_query=coarse_query, coarse_keyval=coarse_keyval, coarse_out=coarse_out, up_weight=up_weight)


epsilon = 1e-06
big_negative = -1e+30

def normalize(values, scale_gain):
    mean_square = lax.optimization_barrier(jnp.mean(values * values, axis=-1, keepdims=True))
    return values * lax.rsqrt(mean_square + epsilon) * scale_gain

def fine_attention(queries, keyvals):
    total_rows = queries.shape[0]
    heads = D_FINE // HEAD
    scale = 1.0 / math.sqrt(HEAD)
    query_heads = queries.reshape(total_rows, heads, HEAD)
    padded = jnp.concatenate([jnp.zeros((WINDOW, 2 * D_FINE), jnp.bfloat16), keyvals], 0)

    def block_step(block):
        first = block * WINDOW
        query_block = lax.dynamic_slice_in_dim(query_heads, first, WINDOW, 0)
        key_block = lax.dynamic_slice_in_dim(padded, first, 2 * WINDOW, 0)
        key_heads = key_block[:, :D_FINE].reshape(2 * WINDOW, heads, HEAD)
        value_heads = key_block[:, D_FINE:].reshape(2 * WINDOW, heads, HEAD)
        scores = jnp.einsum('qhd,khd->hqk', query_block.astype(jnp.float32), key_heads.astype(jnp.float32)) * scale
        row_index = jnp.arange(WINDOW, dtype=jnp.int32)[:, None]
        col_index = jnp.arange(2 * WINDOW, dtype=jnp.int32)[None, :]
        offset = row_index + WINDOW - col_index
        allowed = (offset >= 0) & (offset < WINDOW) & (first - WINDOW + col_index >= 0)
        scores = jnp.where(allowed[None], scores, big_negative)
        peak = lax.optimization_barrier(jnp.max(scores, axis=-1, keepdims=True))
        terms = jnp.where(allowed[None], jnp.exp(scores - peak), 0.0)
        denom = lax.optimization_barrier(jnp.sum(terms, axis=-1))
        weights = terms.astype(jnp.bfloat16).astype(jnp.float32)
        mixed = jnp.einsum('hqk,khd->hqd', weights, value_heads.astype(jnp.float32)) / denom[..., None]
        return jnp.transpose(mixed, (1, 0, 2)).reshape(WINDOW, D_FINE).astype(jnp.bfloat16)
    blocks = lax.map(block_step, jnp.arange(total_rows // WINDOW, dtype=jnp.int32))
    return blocks.reshape(total_rows, D_FINE)

def coarse_attention(queries, keyvals):
    count = queries.shape[0]
    heads = D_COARSE // HEAD
    scale = 1.0 / math.sqrt(HEAD)
    block = 1024 if count % 1024 == 0 else count

    def head_step(head):
        query_head = lax.dynamic_slice_in_dim(queries, head * HEAD, HEAD, 1).astype(jnp.float32)
        key_head = lax.dynamic_slice_in_dim(keyvals, head * HEAD, HEAD, 1).astype(jnp.float32)
        value_head = lax.dynamic_slice_in_dim(keyvals, D_COARSE + head * HEAD, HEAD, 1).astype(jnp.float32)

        def query_step(index):
            first = index * block
            query_block = lax.dynamic_slice_in_dim(query_head, first, block, 0)
            scores = jnp.dot(query_block, key_head.T) * scale
            row_index = first + jnp.arange(block, dtype=jnp.int32)[:, None]
            col_index = jnp.arange(count, dtype=jnp.int32)[None, :]
            allowed = col_index <= row_index
            scores = jnp.where(allowed, scores, big_negative)
            peak = lax.optimization_barrier(jnp.max(scores, axis=-1, keepdims=True))
            terms = jnp.where(allowed, jnp.exp(scores - peak), 0.0)
            denom = lax.optimization_barrier(jnp.sum(terms, axis=-1, keepdims=True))
            weights = terms.astype(jnp.bfloat16).astype(jnp.float32)
            return (jnp.dot(weights, value_head) / denom).astype(jnp.bfloat16)
        outputs = lax.map(query_step, jnp.arange(count // block, dtype=jnp.int32))
        return outputs.reshape(count, HEAD)
    per_head = lax.map(head_step, jnp.arange(heads, dtype=jnp.int32))
    return jnp.transpose(per_head, (1, 0, 2)).reshape(count, D_COARSE)

def reference(tokens, fine_gain, fine_query, fine_keyval, fine_out, down_weight, coarse_gain, coarse_query, coarse_keyval, coarse_out, up_weight):
    inputs = tokens.astype(jnp.float32)
    normed = normalize(inputs, fine_gain).astype(jnp.bfloat16)
    queries = jnp.dot(normed, fine_query, preferred_element_type=jnp.float32).astype(jnp.bfloat16)
    keyvals = jnp.dot(normed, fine_keyval, preferred_element_type=jnp.float32).astype(jnp.bfloat16)
    local = fine_attention(queries, keyvals)
    fine_state = (inputs + jnp.dot(local, fine_out, preferred_element_type=jnp.float32)).astype(jnp.bfloat16)
    count = fine_state.shape[0] // SHORT
    pooled = lax.optimization_barrier(jnp.mean(fine_state.astype(jnp.float32).reshape(count, SHORT, D_FINE), axis=1)).astype(jnp.bfloat16)
    shortened = jnp.dot(pooled, down_weight, preferred_element_type=jnp.float32).astype(jnp.bfloat16)
    coarse_normed = normalize(shortened.astype(jnp.float32), coarse_gain).astype(jnp.bfloat16)
    coarse_queries = jnp.dot(coarse_normed, coarse_query, preferred_element_type=jnp.float32).astype(jnp.bfloat16)
    coarse_kv = jnp.dot(coarse_normed, coarse_keyval.reshape(D_COARSE, 2 * D_COARSE), preferred_element_type=jnp.float32).astype(jnp.bfloat16)
    coarse_heads = coarse_attention(coarse_queries, coarse_kv)
    coarse_state = (shortened.astype(jnp.float32) + jnp.dot(coarse_heads, coarse_out, preferred_element_type=jnp.float32)).astype(jnp.bfloat16)
    delayed = jnp.concatenate([jnp.zeros((1, D_COARSE), jnp.bfloat16), coarse_state[:-1]], 0)
    lifted = jnp.dot(delayed, up_weight, preferred_element_type=jnp.float32)
    result = fine_state.astype(jnp.float32) + jnp.repeat(lifted, SHORT, axis=0)
    return result.astype(jnp.bfloat16)
```

```python
import math

import jax
import jax.numpy as jnp
from jax import lax
from jax.sharding import PartitionSpec as P

HEAD = 128
WINDOW = 256
SHORT = 8


epsilon = 1e-06
big_negative = -1e30


def from_behind(array, axis, by):
    size = lax.axis_size(axis)
    pairs = [(i, i + by) for i in range(size) if 0 <= i + by < size]
    return lax.ppermute(array, axis, pairs)


def normalize(values, scale_gain):
    mean_square = jnp.mean(values * values, axis=-1, keepdims=True)
    return values * lax.rsqrt(mean_square + epsilon) * scale_gain


def online_update(state, query_heads, key_piece, value_piece, query_index):
    running_max, running_sum, accumulate = state
    scale = 1.0 / math.sqrt(HEAD)
    scores = (
        jnp.einsum("qhd,khd->hqk", query_heads, key_piece, preferred_element_type=jnp.float32)
        * scale
    )
    key_index = jnp.arange(key_piece.shape[0], dtype=jnp.int32)
    allowed = key_index[None, :] <= query_index[:, None]
    scores = jnp.where(allowed[None], scores, big_negative)
    new_max = jnp.maximum(running_max, jnp.max(scores, axis=-1))
    terms = jnp.where(allowed[None], jnp.exp(scores - new_max[..., None]), 0.0)
    new_sum = jnp.sum(terms, axis=-1)
    product = jnp.einsum(
        "hqk,khd->hqd", terms.astype(jnp.bfloat16), value_piece, preferred_element_type=jnp.float32
    )
    return (new_max, new_sum, product)


def body(
    tokens,
    fine_gain,
    fine_query,
    fine_keyval,
    fine_out,
    down_weight,
    coarse_gain,
    coarse_query,
    coarse_keyval,
    coarse_out,
    up_weight,
):
    tok_rows = tokens.shape[0]
    width = tokens.shape[1]
    fine_heads = width // HEAD
    scale = 1.0 / math.sqrt(HEAD)
    start_row = lax.axis_index(("seq", "tp")) * tok_rows
    inputs = tokens.astype(jnp.float32)
    normed = normalize(inputs, fine_gain).astype(jnp.bfloat16)
    queries = jnp.dot(normed, fine_query, preferred_element_type=jnp.float32).astype(jnp.bfloat16)
    keyvals = jnp.dot(normed, fine_keyval, preferred_element_type=jnp.float32).astype(jnp.bfloat16)
    earlier = from_behind(keyvals, ("seq", "tp"), 1)
    key_rows = jnp.concatenate([earlier, keyvals], 0)
    span = key_rows.shape[0]
    key_heads = key_rows[:, :width].reshape(span, fine_heads, HEAD)
    value_heads = key_rows[:, width:].reshape(span, fine_heads, HEAD)
    query_heads = queries.reshape(tok_rows, fine_heads, HEAD)
    scores = (
        jnp.einsum("qhd,khd->hqk", query_heads, key_heads, preferred_element_type=jnp.float32)
        * scale
    )
    row_index = jnp.arange(tok_rows, dtype=jnp.int32)[:, None]
    col_index = jnp.arange(span, dtype=jnp.int32)[None, :]
    offset = row_index + WINDOW - col_index
    allowed = (offset >= 0) & (offset < WINDOW) & (start_row - WINDOW + col_index >= 0)
    scores = jnp.where(allowed[None], scores, big_negative)
    peak = jnp.max(scores, axis=-1, keepdims=True)
    terms = jnp.where(allowed[None], jnp.exp(scores - peak), 0.0)
    denom = jnp.sum(terms, axis=-1)
    mixed = jnp.einsum(
        "hqk,khd->qhd", terms.astype(jnp.bfloat16), value_heads, preferred_element_type=jnp.float32
    )
    local = (mixed / jnp.transpose(denom)[..., None]).reshape(tok_rows, width).astype(jnp.bfloat16)
    fine_state = (inputs + jnp.dot(local, fine_out, preferred_element_type=jnp.float32)).astype(
        jnp.bfloat16
    )
    pooled = jnp.mean(
        fine_state.astype(jnp.float32).reshape(tok_rows // SHORT, SHORT, width), axis=1
    ).astype(jnp.bfloat16)
    pooled_all = lax.all_gather(pooled, "tp", axis=0, tiled=True)
    short_cols = jnp.dot(pooled_all, down_weight, preferred_element_type=jnp.float32).astype(
        jnp.bfloat16
    )
    shortened = lax.all_gather(short_cols, "tp", axis=1, tiled=True)
    coarse_normed = normalize(shortened.astype(jnp.float32), coarse_gain).astype(jnp.bfloat16)
    coarse_rows = coarse_normed.shape[0]
    local_cols = coarse_query.shape[1]
    local_heads = local_cols // HEAD
    query_rows = lax.all_gather(coarse_query, "seq", axis=0, tiled=True)
    keyval_rows = lax.all_gather(coarse_keyval, "seq", axis=0, tiled=True)
    count = query_rows.shape[0]
    query_sum = jnp.dot(coarse_normed, query_rows, preferred_element_type=jnp.float32)
    keyval_sum = jnp.dot(
        coarse_normed,
        keyval_rows.reshape(count, 2 * local_cols),
        preferred_element_type=jnp.float32,
    )
    coarse_queries = query_sum.astype(jnp.bfloat16).reshape(coarse_rows, local_heads, HEAD)
    coarse_kv = keyval_sum.astype(jnp.bfloat16).reshape(coarse_rows, 2, local_cols)
    my_first = lax.axis_index("seq") * coarse_rows
    query_index = my_first + jnp.arange(coarse_rows, dtype=jnp.int32)
    initial = (
        jnp.full((local_heads, coarse_rows), big_negative, jnp.float32),
        jnp.zeros((local_heads, coarse_rows), jnp.float32),
        jnp.zeros((local_heads, coarse_rows, HEAD), jnp.float32),
    )
    piece = lax.all_gather(coarse_kv, "seq", axis=0, tiled=True)
    count = piece.shape[0]
    key_piece = piece[:, 0].reshape(count, local_heads, HEAD)
    value_piece = piece[:, 1].reshape(count, local_heads, HEAD)
    final = lax.cond(
        jnp.int32(0) < my_first + coarse_rows,
        lambda: online_update(initial, coarse_queries, key_piece, value_piece, query_index),
        lambda: initial,
    )
    head_out = final[2] / final[1][..., None]
    coarse_heads = (
        jnp.transpose(head_out, (1, 0, 2)).reshape(coarse_rows, local_cols).astype(jnp.bfloat16)
    )
    partials = jnp.dot(coarse_heads, coarse_out, preferred_element_type=jnp.float32)
    attended = lax.psum_scatter(
        partials.astype(jnp.bfloat16), "tp", scatter_dimension=1, tiled=True
    ).astype(jnp.float32)
    coarse_state = (short_cols.astype(jnp.float32) + attended).astype(jnp.bfloat16)
    prior_row = from_behind(coarse_state[coarse_rows - 1 :], "seq", 1)
    delayed = jnp.concatenate([prior_row, coarse_state[: coarse_rows - 1]], 0)
    lifted = lax.psum_scatter(
        jnp.dot(delayed, up_weight, preferred_element_type=jnp.float32).astype(jnp.bfloat16),
        "tp",
        scatter_dimension=0,
        tiled=True,
    ).astype(jnp.float32)
    result = fine_state.astype(jnp.float32) + jnp.repeat(lifted, SHORT, axis=0)
    return result.astype(jnp.bfloat16)


def head_attention(queries, keys, values):
    count, columns = queries.shape
    heads = columns // HEAD
    scale = 1.0 / math.sqrt(HEAD)
    outs = []
    index = jnp.arange(count, dtype=jnp.int32)
    allowed = index[None, :] <= index[:, None]
    for head in range(heads):
        part = slice(head * HEAD, (head + 1) * HEAD)
        scores = (
            jnp.dot(queries[:, part], keys[:, part].T, preferred_element_type=jnp.float32) * scale
        )
        scores = jnp.where(allowed, scores, big_negative)
        peak = jnp.max(scores, axis=-1, keepdims=True)
        terms = jnp.where(allowed, jnp.exp(scores - peak), 0.0)
        denom = jnp.sum(terms, axis=-1, keepdims=True)
        mixed = jnp.dot(
            terms.astype(jnp.bfloat16), values[:, part], preferred_element_type=jnp.float32
        )
        outs.append((mixed / denom).astype(jnp.bfloat16))
    return jnp.concatenate(outs, 1)


def head_body(
    tokens,
    fine_gain,
    fine_query,
    fine_keyval,
    fine_out,
    down_weight,
    coarse_gain,
    coarse_query,
    coarse_keyval,
    coarse_out,
    up_weight,
):
    seq = lax.axis_size("seq")
    tok_rows, width = tokens.shape
    fine_heads = width // HEAD
    scale = 1.0 / math.sqrt(HEAD)
    start_row = lax.axis_index(("seq", "tp")) * tok_rows
    earlier = from_behind(tokens, ("seq", "tp"), 1)
    down_all = lax.all_gather(down_weight, "tp", axis=1, tiled=True)
    depth, local_cols = coarse_query.shape
    own = local_cols // seq
    stacked = jnp.concatenate(
        [
            coarse_query.reshape(depth, 1, seq, own),
            coarse_keyval.reshape(depth, 2, seq, own),
        ],
        1,
    )
    stacked = jnp.transpose(stacked, (2, 0, 1, 3)).reshape(seq, depth, 3 * own)
    weights = lax.all_to_all(stacked, "seq", 0, 0, tiled=True).reshape(seq * depth, 3 * own)
    both = jnp.concatenate([earlier, tokens], 0).astype(jnp.float32)
    normed = normalize(both, fine_gain).astype(jnp.bfloat16)
    inputs = tokens.astype(jnp.float32)
    queries = jnp.dot(
        normed[tok_rows:], fine_query, preferred_element_type=jnp.float32
    ).astype(jnp.bfloat16)
    key_rows = jnp.dot(normed, fine_keyval, preferred_element_type=jnp.float32).astype(jnp.bfloat16)
    span = key_rows.shape[0]
    key_heads = key_rows[:, :width].reshape(span, fine_heads, HEAD)
    value_heads = key_rows[:, width:].reshape(span, fine_heads, HEAD)
    query_heads = queries.reshape(tok_rows, fine_heads, HEAD)
    scores = (
        jnp.einsum("qhd,khd->hqk", query_heads, key_heads, preferred_element_type=jnp.float32)
        * scale
    )
    row_index = jnp.arange(tok_rows, dtype=jnp.int32)[:, None]
    col_index = jnp.arange(span, dtype=jnp.int32)[None, :]
    offset = row_index + WINDOW - col_index
    allowed = (offset >= 0) & (offset < WINDOW) & (start_row - WINDOW + col_index >= 0)
    scores = jnp.where(allowed[None], scores, big_negative)
    peak = jnp.max(scores, axis=-1, keepdims=True)
    terms = jnp.where(allowed[None], jnp.exp(scores - peak), 0.0)
    denom = jnp.sum(terms, axis=-1)
    mixed = jnp.einsum(
        "hqk,khd->qhd", terms.astype(jnp.bfloat16), value_heads, preferred_element_type=jnp.float32
    )
    local = (mixed / jnp.transpose(denom)[..., None]).reshape(tok_rows, width).astype(jnp.bfloat16)
    fine_state = (inputs + jnp.dot(local, fine_out, preferred_element_type=jnp.float32)).astype(
        jnp.bfloat16
    )
    pooled = jnp.mean(
        fine_state.astype(jnp.float32).reshape(tok_rows // SHORT, SHORT, width), axis=1
    ).astype(jnp.bfloat16)
    pooled_all = lax.all_gather(pooled, ("seq", "tp"), axis=0, tiled=True)
    shortened = jnp.dot(pooled_all, down_all, preferred_element_type=jnp.float32).astype(
        jnp.bfloat16
    )
    coarse_normed = normalize(shortened.astype(jnp.float32), coarse_gain).astype(jnp.bfloat16)
    projected = jnp.dot(coarse_normed, weights, preferred_element_type=jnp.float32).astype(
        jnp.bfloat16
    )
    heads_out = head_attention(
        projected[:, :own], projected[:, own : 2 * own], projected[:, 2 * own :]
    )
    count = heads_out.shape[0]
    coarse_rows = count // seq
    coarse_heads = lax.all_to_all(
        heads_out.reshape(seq, coarse_rows, own), "seq", 0, 0, tiled=True
    )
    coarse_heads = jnp.transpose(coarse_heads, (1, 0, 2)).reshape(coarse_rows, local_cols)
    short_cols = lax.dynamic_slice(
        shortened,
        (lax.axis_index("seq") * coarse_rows, lax.axis_index("tp") * local_cols),
        (coarse_rows, local_cols),
    )
    partials = jnp.dot(coarse_heads, coarse_out, preferred_element_type=jnp.float32)
    attended = lax.psum_scatter(
        partials.astype(jnp.bfloat16), "tp", scatter_dimension=1, tiled=True
    ).astype(jnp.float32)
    coarse_state = (short_cols.astype(jnp.float32) + attended).astype(jnp.bfloat16)
    prior_row = from_behind(coarse_state[coarse_rows - 1 :], "seq", 1)
    delayed = jnp.concatenate([prior_row, coarse_state[: coarse_rows - 1]], 0)
    lifted = lax.psum_scatter(
        jnp.dot(delayed, up_weight, preferred_element_type=jnp.float32).astype(jnp.bfloat16),
        "tp",
        scatter_dimension=0,
        tiled=True,
    ).astype(jnp.float32)
    result = fine_state.astype(jnp.float32) + jnp.repeat(lifted, SHORT, axis=0)
    return result.astype(jnp.bfloat16)


def chosen(*args):
    local_heads = args[7].shape[1] // HEAD
    if local_heads % lax.axis_size("seq") == 0 and args[0].shape[0] == WINDOW:
        return head_body(*args)
    return body(*args)


def solution(mesh):
    return jax.shard_map(
        chosen,
        mesh=mesh,
        in_specs=(
            P(("seq", "tp"), None),
            P(),
            P(),
            P(),
            P(),
            P(None, "tp"),
            P(),
            P("seq", "tp"),
            P("seq", None, "tp"),
            P("tp", None),
            P("tp", None),
        ),
        out_specs=P(("seq", "tp"), None),
        check_vma=False,
    )
```

```python
import functools
import math

import jax
import jax.numpy as jnp
from jax import lax
from jax.experimental import pallas as pl
from jax.experimental.pallas import tpu as pltpu
from jax.sharding import PartitionSpec as P

HEAD = 128
WINDOW = 256
SHORT = 8


epsilon = 1e-06
big_negative = -1e30


def from_behind(array, axis, by):
    size = lax.axis_size(axis)
    pairs = [(i, i + by) for i in range(size) if 0 <= i + by < size]
    return lax.ppermute(array, axis, pairs)


def normalize(values, scale_gain):
    mean_square = jnp.mean(values * values, axis=-1, keepdims=True)
    return values * lax.rsqrt(mean_square + epsilon) * scale_gain


def online_update(state, query_heads, key_piece, value_piece, query_index):
    running_max, running_sum, accumulate = state
    scale = 1.0 / math.sqrt(HEAD)
    scores = (
        jnp.einsum("qhd,khd->hqk", query_heads, key_piece, preferred_element_type=jnp.float32)
        * scale
    )
    key_index = jnp.arange(key_piece.shape[0], dtype=jnp.int32)
    allowed = key_index[None, :] <= query_index[:, None]
    scores = jnp.where(allowed[None], scores, big_negative)
    new_max = jnp.maximum(running_max, jnp.max(scores, axis=-1))
    terms = jnp.where(allowed[None], jnp.exp(scores - new_max[..., None]), 0.0)
    new_sum = jnp.sum(terms, axis=-1)
    product = jnp.einsum(
        "hqk,khd->hqd", terms.astype(jnp.bfloat16), value_piece, preferred_element_type=jnp.float32
    )
    return (new_max, new_sum, product)


def body(
    tokens,
    fine_gain,
    fine_query,
    fine_keyval,
    fine_out,
    down_weight,
    coarse_gain,
    coarse_query,
    coarse_keyval,
    coarse_out,
    up_weight,
):
    tok_rows = tokens.shape[0]
    width = tokens.shape[1]
    fine_heads = width // HEAD
    scale = 1.0 / math.sqrt(HEAD)
    start_row = lax.axis_index(("seq", "tp")) * tok_rows
    inputs = tokens.astype(jnp.float32)
    normed = normalize(inputs, fine_gain).astype(jnp.bfloat16)
    queries = jnp.dot(normed, fine_query, preferred_element_type=jnp.float32).astype(jnp.bfloat16)
    keyvals = jnp.dot(normed, fine_keyval, preferred_element_type=jnp.float32).astype(jnp.bfloat16)
    earlier = from_behind(keyvals, ("seq", "tp"), 1)
    key_rows = jnp.concatenate([earlier, keyvals], 0)
    span = key_rows.shape[0]
    key_heads = key_rows[:, :width].reshape(span, fine_heads, HEAD)
    value_heads = key_rows[:, width:].reshape(span, fine_heads, HEAD)
    query_heads = queries.reshape(tok_rows, fine_heads, HEAD)
    scores = (
        jnp.einsum("qhd,khd->hqk", query_heads, key_heads, preferred_element_type=jnp.float32)
        * scale
    )
    row_index = jnp.arange(tok_rows, dtype=jnp.int32)[:, None]
    col_index = jnp.arange(span, dtype=jnp.int32)[None, :]
    offset = row_index + WINDOW - col_index
    allowed = (offset >= 0) & (offset < WINDOW) & (start_row - WINDOW + col_index >= 0)
    scores = jnp.where(allowed[None], scores, big_negative)
    peak = jnp.max(scores, axis=-1, keepdims=True)
    terms = jnp.where(allowed[None], jnp.exp(scores - peak), 0.0)
    denom = jnp.sum(terms, axis=-1)
    mixed = jnp.einsum(
        "hqk,khd->qhd", terms.astype(jnp.bfloat16), value_heads, preferred_element_type=jnp.float32
    )
    local = (mixed / jnp.transpose(denom)[..., None]).reshape(tok_rows, width).astype(jnp.bfloat16)
    fine_state = (inputs + jnp.dot(local, fine_out, preferred_element_type=jnp.float32)).astype(
        jnp.bfloat16
    )
    pooled = jnp.mean(
        fine_state.astype(jnp.float32).reshape(tok_rows // SHORT, SHORT, width), axis=1
    ).astype(jnp.bfloat16)
    pooled_all = lax.all_gather(pooled, "tp", axis=0, tiled=True)
    short_cols = jnp.dot(pooled_all, down_weight, preferred_element_type=jnp.float32).astype(
        jnp.bfloat16
    )
    shortened = lax.all_gather(short_cols, "tp", axis=1, tiled=True)
    coarse_normed = normalize(shortened.astype(jnp.float32), coarse_gain).astype(jnp.bfloat16)
    coarse_rows = coarse_normed.shape[0]
    local_cols = coarse_query.shape[1]
    local_heads = local_cols // HEAD
    query_rows = lax.all_gather(coarse_query, "seq", axis=0, tiled=True)
    keyval_rows = lax.all_gather(coarse_keyval, "seq", axis=0, tiled=True)
    count = query_rows.shape[0]
    query_sum = jnp.dot(coarse_normed, query_rows, preferred_element_type=jnp.float32)
    keyval_sum = jnp.dot(
        coarse_normed,
        keyval_rows.reshape(count, 2 * local_cols),
        preferred_element_type=jnp.float32,
    )
    coarse_queries = query_sum.astype(jnp.bfloat16).reshape(coarse_rows, local_heads, HEAD)
    coarse_kv = keyval_sum.astype(jnp.bfloat16).reshape(coarse_rows, 2, local_cols)
    my_first = lax.axis_index("seq") * coarse_rows
    query_index = my_first + jnp.arange(coarse_rows, dtype=jnp.int32)
    initial = (
        jnp.full((local_heads, coarse_rows), big_negative, jnp.float32),
        jnp.zeros((local_heads, coarse_rows), jnp.float32),
        jnp.zeros((local_heads, coarse_rows, HEAD), jnp.float32),
    )
    piece = lax.all_gather(coarse_kv, "seq", axis=0, tiled=True)
    count = piece.shape[0]
    key_piece = piece[:, 0].reshape(count, local_heads, HEAD)
    value_piece = piece[:, 1].reshape(count, local_heads, HEAD)
    final = lax.cond(
        jnp.int32(0) < my_first + coarse_rows,
        lambda: online_update(initial, coarse_queries, key_piece, value_piece, query_index),
        lambda: initial,
    )
    head_out = final[2] / final[1][..., None]
    coarse_heads = (
        jnp.transpose(head_out, (1, 0, 2)).reshape(coarse_rows, local_cols).astype(jnp.bfloat16)
    )
    partials = jnp.dot(coarse_heads, coarse_out, preferred_element_type=jnp.float32)
    attended = lax.psum_scatter(
        partials.astype(jnp.bfloat16), "tp", scatter_dimension=1, tiled=True
    ).astype(jnp.float32)
    coarse_state = (short_cols.astype(jnp.float32) + attended).astype(jnp.bfloat16)
    prior_row = from_behind(coarse_state[coarse_rows - 1 :], "seq", 1)
    delayed = jnp.concatenate([prior_row, coarse_state[: coarse_rows - 1]], 0)
    lifted = lax.psum_scatter(
        jnp.dot(delayed, up_weight, preferred_element_type=jnp.float32).astype(jnp.bfloat16),
        "tp",
        scatter_dimension=0,
        tiled=True,
    ).astype(jnp.float32)
    result = fine_state.astype(jnp.float32) + jnp.repeat(lifted, SHORT, axis=0)
    return result.astype(jnp.bfloat16)


def flip(index, bit):
    return index + bit - 2 * bit * lax.rem(lax.div(index, jnp.int32(bit)), jnp.int32(2))


def bits_of(size):
    out, bit = [], size // 2
    while bit:
        out.append(bit)
        bit //= 2
    return out


def dot32(left, right):
    return jnp.dot(left, right, preferred_element_type=jnp.float32)


def dot_t(left, right):
    return lax.dot_general(
        left, right, (((1,), (1,)), ((), ())), preferred_element_type=jnp.float32
    )


def section_kernel(
    seq, tp,
    tokens, fine_gain, fine_query, fine_keyval, fine_out, down_weight, coarse_gain, stacked,
    coarse_out, up_weight,
    result,
    both, wq, wkv, wo, down_all, weights, wout, wup,
    normed, queries, key_rows, local, fine_state, pooled_all, coarse_normed, projected,
    heads_out, heads_in, coarse_heads, short_cols, send1, recv1, state, prior, send2, recv2,
    load_sem, halo_s, halo_r, w_s, w_r, d_s, d_r, p_s, p_r, h_s, h_r, r1_s, r1_r, row_s, row_r,
    r2_s, r2_r,
):
    me_s = lax.axis_index("seq")
    me_t = lax.axis_index("tp")
    rows, width = tokens.shape
    scale = 1.0 / math.sqrt(HEAD)
    total = seq * tp
    lin = me_s * tp + me_t
    after = lax.rem(lin + 1, total)
    before = lax.rem(lin + total - 1, total)

    def around(index, step, size):
        return lax.rem(index + step, size)

    def remote(src, dst, send, recv, device):
        copy = pltpu.make_async_remote_copy(
            src_ref=src, dst_ref=dst, send_sem=send, recv_sem=recv,
            device_id=device, device_id_type=pl.DeviceIdType.MESH,
        )
        copy.start()
        return copy

    def load(src, dst, index):
        copy = pltpu.make_async_copy(src, dst, load_sem.at[index])
        copy.start()
        return copy

    def linear(index):
        return {"seq": lax.div(index, tp), "tp": lax.rem(index, tp)}

    barrier = pltpu.get_barrier_semaphore()
    peers = [{"seq": around(me_s, d, seq)} for d in range(1, seq)]
    peers += [{"tp": around(me_t, d, tp)} for d in range(1, tp)]
    peers += [linear(after), linear(before)]
    in_tokens = load(tokens, both.at[pl.ds(rows, rows)], 0)
    in_wkv = load(fine_keyval, wkv, 1)
    in_wq = load(fine_query, wq, 2)
    in_wo = load(fine_out, wo, 3)
    in_down = load(down_weight, down_all.at[me_t], 4)
    in_w = load(stacked.at[me_s], weights.at[me_s], 5)
    in_wout = load(coarse_out, wout, 6)
    in_wup = load(up_weight, wup, 7)
    for peer in peers:
        pl.semaphore_signal(barrier, inc=1, device_id=peer, device_id_type=pl.DeviceIdType.MESH)
    pl.semaphore_wait(barrier, len(peers))

    halo = remote(tokens, both.at[pl.ds(0, rows)], halo_s, halo_r, linear(after))
    order = sorted(range(1, seq), key=lambda d: abs(2 * d - seq))
    w_copies = []

    def send_weights(offsets):
        for d in offsets:
            dest = around(me_s, d, seq)
            w_copies.append(
                remote(
                    stacked.at[dest], weights.at[me_s], w_s.at[d - 1], w_r.at[d - 1],
                    {"seq": dest},
                )
            )

    send_weights(order[: (seq + 1) // 2])
    tp_bits = bits_of(tp)
    d_first = [
        remote(
            down_weight, down_all.at[me_t], d_s.at[bit - 1], d_r.at[bit - 1],
            {"tp": flip(me_t, bit)},
        )
        for bit in tp_bits
    ]

    gain = fine_gain[...]

    def norm_rows(first):
        values = both[pl.ds(first, rows), :].astype(jnp.float32)
        normed[pl.ds(first, rows), :] = normalize(values, gain).astype(jnp.bfloat16)

    in_tokens.wait()
    norm_rows(rows)
    in_wq.wait()
    tile = 2 * HEAD

    @pl.loop(0, width // tile)
    def _(i):
        cols = pl.ds(pl.multiple_of(i * tile, tile), tile)
        queries[:, cols] = dot32(normed[rows:, :], wq[:, cols]).astype(jnp.bfloat16)

    halo.wait()
    norm_rows(0)
    in_wkv.wait()

    @pl.loop(0, 2 * width // tile)
    def _(i):
        cols = pl.ds(pl.multiple_of(i * tile, tile), tile)
        key_rows[:, cols] = dot32(normed[...], wkv[:, cols]).astype(jnp.bfloat16)

    row_index = lax.broadcasted_iota(jnp.int32, (rows, 2 * rows), 0)
    col_index = lax.broadcasted_iota(jnp.int32, (rows, 2 * rows), 1)
    offset = row_index + rows - col_index
    allowed = (offset >= 0) & (offset < WINDOW) & (lin * rows - rows + col_index >= 0)

    def attend(query, key, value, mask):
        scores = jnp.where(mask, dot_t(query, key) * scale, big_negative)
        peak = jnp.max(scores, axis=-1, keepdims=True)
        terms = jnp.where(mask, jnp.exp(scores - peak), 0.0)
        denom = jnp.sum(terms, axis=-1, keepdims=True)
        return (dot32(terms.astype(jnp.bfloat16), value) / denom).astype(jnp.bfloat16)

    @pl.loop(0, width // HEAD)
    def _(h):
        cols = pl.ds(pl.multiple_of(h * HEAD, HEAD), HEAD)
        vcols = pl.ds(pl.multiple_of(width + h * HEAD, HEAD), HEAD)
        local[:, cols] = attend(queries[:, cols], key_rows[:, cols], key_rows[:, vcols], allowed)

    in_wo.wait()
    pool_rows = rows // SHORT

    @pl.loop(0, width // tile)
    def _(i):
        cols = pl.ds(pl.multiple_of(i * tile, tile), tile)
        value = both[rows:, cols].astype(jnp.float32) + dot32(local[...], wo[:, cols])
        value = value.astype(jnp.bfloat16)
        fine_state[:, cols] = value
        mean = jnp.mean(value.astype(jnp.float32).reshape(pool_rows, SHORT, tile), axis=1)
        pooled_all[lin, :, cols] = mean.astype(jnp.bfloat16)

    done = []
    held = [lin]
    count = 0
    for axis, bits in (("seq", bits_of(seq)), ("tp", tp_bits)):
        for bit in bits:
            stride = bit * tp if axis == "seq" else bit
            where = {axis: flip(me_s if axis == "seq" else me_t, bit)}
            copies = []
            for slot in held:
                copies.append(
                    remote(
                        pooled_all.at[slot], pooled_all.at[slot], p_s.at[count], p_r.at[count],
                        where,
                    )
                )
                count += 1
            if axis == "tp" and bit == tp_bits[0]:
                send_weights(order[(seq + 1) // 2 :])
            for copy in copies:
                copy.wait_recv()
            done += copies
            held = held + [flip(slot, stride) for slot in held]
    d_done = list(d_first)
    for copy in d_first[:1]:
        copy.wait_recv()
    have = [tp_bits[0]]
    index = tp - 1
    extra = []
    for k, bit in enumerate(tp_bits[1:]):
        subs = list(have)
        now = []
        for sub in subs:
            slot = me_t
            for other in tp_bits:
                if sub & other:
                    slot = flip(slot, other)
            number = bit + sub - 1
            now.append(
                remote(
                    down_all.at[slot], down_all.at[slot], d_s.at[number], d_r.at[number],
                    {"tp": flip(me_t, bit)},
                )
            )
        d_first[k + 1].wait_recv()
        for copy in now:
            copy.wait_recv()
        extra += now
        have = have + [bit] + [bit + sub for sub in subs]
    in_down.wait()

    per = seq // 2 if seq > 1 else 1
    crows = pool_rows * tp
    block = 2 * crows
    cgain = coarse_gain[...]

    @pl.loop(0, seq // 2)
    def _(i):
        first = pl.multiple_of(i * block, block)
        pooled = pooled_all[pl.ds(i * 2 * tp, 2 * tp)].reshape(block, width)
        total_sq = jnp.zeros((block, 1), jnp.float32)
        fcols = down_all.shape[2]
        half = fcols // 2
        for t in range(tp):
            for u in range(2):
                part = dot32(pooled, down_all[t, :, u * half : (u + 1) * half]).astype(jnp.bfloat16)
                wide = part.astype(jnp.float32)
                total_sq += jnp.sum(wide * wide, axis=-1, keepdims=True)
                base = t * fcols + u * half
                coarse_normed[pl.ds(first, block), base : base + half] = part
        factor = lax.rsqrt(total_sq / (tp * fcols) + epsilon)
        for t in range(2 * tp):
            cols = slice(t * half, (t + 1) * half)
            wide = coarse_normed[pl.ds(first, block), cols].astype(jnp.float32)
            coarse_normed[pl.ds(first, block), cols] = (wide * factor * cgain[:, cols]).astype(
                jnp.bfloat16
            )

    mine = pooled_all[pl.ds(me_s * tp, tp)].reshape(crows, width)
    fcols = down_all.shape[2]
    for u in range(2):
        cols = slice(u * fcols // 2, (u + 1) * fcols // 2)
        short_cols[:, cols] = dot32(mine, down_all[me_t, :, cols])
    in_w.wait()
    for copy in w_copies:
        copy.wait_recv()
    depth, three = weights.shape[1:]
    own = three // 3

    @pl.loop(0, seq // 2)
    def _(i):
        first = pl.multiple_of(i * block, block)
        acc = jnp.zeros((block, three), jnp.float32)
        for j in range(seq):
            acc += dot32(
                coarse_normed[pl.ds(first, block), j * depth : (j + 1) * depth], weights[j]
            )
        projected[pl.ds(first, block), :] = acc.astype(jnp.bfloat16)

    for i in range(seq // 2):
        extent = (i + 1) * block
        r = lax.broadcasted_iota(jnp.int32, (block, extent), 0) + i * block
        c = lax.broadcasted_iota(jnp.int32, (block, extent), 1)
        for h in range(own // HEAD):
            part = slice(h * HEAD, (h + 1) * HEAD)
            kpart = slice(own + h * HEAD, own + (h + 1) * HEAD)
            vpart = slice(2 * own + h * HEAD, 2 * own + (h + 1) * HEAD)
            out = attend(
                projected[i * block : extent, part], projected[:extent, kpart],
                projected[:extent, vpart], c <= r,
            )
            heads_out[2 * i : 2 * i + 2, :, part] = out.reshape(2, crows, HEAD)

    heads_in[me_s] = heads_out[me_s]
    h_copies = []
    for d in order:
        dest = around(me_s, d, seq)
        h_copies.append(
            remote(
                heads_out.at[dest], heads_in.at[me_s], h_s.at[d - 1], h_r.at[d - 1],
                {"seq": dest},
            )
        )
    in_wout.wait()
    in_wup.wait()
    for copy in h_copies:
        copy.wait_recv()
    for j in range(seq):
        coarse_heads[:, j * own : (j + 1) * own] = heads_in[j]

    def partial(t, store):
        @pl.loop(0, fcols // tile)
        def _(i):
            cols = pl.ds(pl.multiple_of(i * tile, tile), tile)
            wcols = pl.ds(pl.multiple_of(t * fcols + i * tile, tile), tile)
            store(cols, dot32(coarse_heads[...], wout[:, wcols]))

    tp_order = sorted(range(1, tp), key=lambda d: abs(2 * d - tp))
    r1 = []
    for d in tp_order:
        dest = around(me_t, d, tp)

        def put(cols, value, d=d):
            send1[d - 1, :, cols] = value.astype(jnp.bfloat16)

        partial(dest, put)
        r1.append(
            remote(
                send1.at[d - 1], recv1.at[d - 1], r1_s.at[d - 1], r1_r.at[d - 1], {"tp": dest}
            )
        )

    def keep(cols, value):
        short_cols[:, cols] = short_cols[:, cols].astype(jnp.bfloat16).astype(jnp.float32) + value

    partial(me_t, keep)
    for copy in r1:
        copy.wait_recv()
    whole = short_cols[...]
    for d in range(1, tp):
        whole += recv1[d - 1].astype(jnp.float32)
    state[...] = whole.astype(jnp.bfloat16)
    slab = prior.shape[0]
    row_copy = remote(
        state.at[pl.ds(crows - slab, slab)], prior, row_s, row_r, {"seq": around(me_s, 1, seq)}
    )
    rolled = pltpu.roll(state[...].astype(jnp.float32), 1, 0)
    row_copy.wait_recv()
    previous = prior[...].astype(jnp.float32)[slab - 1 : slab, :]
    previous = jnp.where(me_s > 0, previous, 0.0)
    top = lax.broadcasted_iota(jnp.int32, rolled.shape, 0) == 0
    delayed = jnp.where(top, previous, rolled).astype(jnp.bfloat16)
    coarse_heads[...] = delayed

    @pl.loop(0, width // tile)
    def _(i):
        cols = pl.ds(pl.multiple_of(i * tile, tile), tile)
        short_cols[:, cols] = dot32(coarse_heads[...], wup[:, cols])

    r2 = []
    for d in tp_order:
        dest = around(me_t, d, tp)
        part = short_cols[pl.ds(pl.multiple_of(dest * pool_rows, pool_rows), pool_rows), :]
        send2[d - 1] = part.astype(jnp.bfloat16)
        r2.append(
            remote(
                send2.at[d - 1], recv2.at[d - 1], r2_s.at[d - 1], r2_r.at[d - 1], {"tp": dest}
            )
        )
    lifted = short_cols[pl.ds(pl.multiple_of(me_t * pool_rows, pool_rows), pool_rows), :]
    for copy in r2:
        copy.wait_recv()
    for d in range(1, tp):
        lifted += recv2[d - 1].astype(jnp.float32)
    spread = jnp.broadcast_to(lifted[:, None, :], (pool_rows, SHORT, width)).reshape(rows, width)
    result[...] = (fine_state[...].astype(jnp.float32) + spread).astype(jnp.bfloat16)
    for copy in w_copies + d_done + extra + done + h_copies + r1 + [row_copy] + r2:
        copy.wait_send()


def head_body(
    tokens,
    fine_gain,
    fine_query,
    fine_keyval,
    fine_out,
    down_weight,
    coarse_gain,
    coarse_query,
    coarse_keyval,
    coarse_out,
    up_weight,
):
    seq, tp = lax.axis_size("seq"), lax.axis_size("tp")
    rows, width = tokens.shape
    depth, local_cols = coarse_query.shape
    own = local_cols // seq
    stacked = jnp.concatenate(
        [
            coarse_query.reshape(depth, 1, seq, own),
            coarse_keyval.reshape(depth, 2, seq, own),
        ],
        1,
    )
    stacked = jnp.transpose(stacked, (2, 0, 1, 3)).reshape(seq, depth, 3 * own)
    pool_rows = rows // SHORT
    crows = pool_rows * tp
    count = crows * seq
    bf, f32 = jnp.bfloat16, jnp.float32
    V = pltpu.VMEM
    dma = lambda n: pltpu.SemaphoreType.DMA((n,))
    one = pltpu.SemaphoreType.DMA
    anywhere = pl.BlockSpec(memory_space=pl.ANY)
    vmem = pl.BlockSpec(memory_space=pltpu.VMEM)
    return pl.pallas_call(
        functools.partial(section_kernel, seq, tp),
        out_shape=jax.ShapeDtypeStruct((rows, width), bf),
        in_specs=[anywhere, vmem, anywhere, anywhere, anywhere, anywhere, vmem, anywhere,
                  anywhere, anywhere],
        out_specs=vmem,
        scratch_shapes=[
            V((2 * rows, width), bf), V(fine_query.shape, bf), V(fine_keyval.shape, bf),
            V(fine_out.shape, bf), V((tp,) + down_weight.shape, bf), V((seq, depth, 3 * own), bf),
            V(coarse_out.shape, bf), V(up_weight.shape, bf),
            V((2 * rows, width), bf), V((rows, width), bf), V((2 * rows, 2 * width), bf),
            V((rows, width), bf), V((rows, width), bf), V((seq * tp, pool_rows, width), bf),
            V((count, tp * local_cols), bf), V((count, 3 * own), bf),
            V((seq, crows, own), bf), V((seq, crows, own), bf), V((crows, local_cols), bf),
            V((crows, local_cols), f32), V((tp - 1, crows, local_cols), bf),
            V((tp - 1, crows, local_cols), bf), V((crows, local_cols), bf), V((16, local_cols), bf),
            V((tp - 1, pool_rows, width), bf), V((tp - 1, pool_rows, width), bf),
            dma(8), one(()), one(()), dma(seq - 1), dma(seq - 1), dma(tp - 1), dma(tp - 1),
            dma(seq * tp - 1), dma(seq * tp - 1), dma(seq - 1), dma(seq - 1),
            dma(tp - 1), dma(tp - 1), one(()), one(()), dma(tp - 1), dma(tp - 1),
        ],
        compiler_params=pltpu.CompilerParams(
            collective_id=0, has_side_effects=True, vmem_limit_bytes=62 * 1024 * 1024
        ),
    )(tokens, fine_gain[None], fine_query, fine_keyval, fine_out, down_weight, coarse_gain[None],
      stacked, coarse_out, up_weight)


def chosen(*args):
    seq, tp = lax.axis_size("seq"), lax.axis_size("tp")
    local_heads = args[7].shape[1] // HEAD
    powers = seq & (seq - 1) == 0 and tp & (tp - 1) == 0 and seq > 1 and tp > 1
    square = args[10].shape[0] == args[10].shape[1] == args[7].shape[1]
    if local_heads % seq == 0 and args[0].shape[0] == WINDOW and powers and square:
        return head_body(*args)
    return body(*args)


def solution(mesh):
    return jax.shard_map(
        chosen,
        mesh=mesh,
        in_specs=(
            P(("seq", "tp"), None),
            P(),
            P(),
            P(),
            P(),
            P(None, "tp"),
            P(),
            P("seq", "tp"),
            P("seq", None, "tp"),
            P("tp", None),
            P("tp", None),
        ),
        out_specs=P(("seq", "tp"), None),
        check_vma=False,
    )
```

```python
import functools
import math

import jax
import jax.numpy as jnp
from jax import lax
from jax.experimental import pallas as pl
from jax.experimental.pallas import tpu as pltpu
from jax.sharding import PartitionSpec as P

HEAD = 128
WINDOW = 256
SHORT = 8


epsilon = 1e-06
big_negative = -1e30


def from_behind(array, axis, by):
    size = lax.axis_size(axis)
    pairs = [(i, i + by) for i in range(size) if 0 <= i + by < size]
    return lax.ppermute(array, axis, pairs)


def normalize(values, scale_gain):
    mean_square = jnp.mean(values * values, axis=-1, keepdims=True)
    return values * lax.rsqrt(mean_square + epsilon) * scale_gain


def online_update(state, query_heads, key_piece, value_piece, query_index):
    running_max, running_sum, accumulate = state
    scale = 1.0 / math.sqrt(HEAD)
    scores = (
        jnp.einsum("qhd,khd->hqk", query_heads, key_piece, preferred_element_type=jnp.float32)
        * scale
    )
    key_index = jnp.arange(key_piece.shape[0], dtype=jnp.int32)
    allowed = key_index[None, :] <= query_index[:, None]
    scores = jnp.where(allowed[None], scores, big_negative)
    new_max = jnp.maximum(running_max, jnp.max(scores, axis=-1))
    terms = jnp.where(allowed[None], jnp.exp(scores - new_max[..., None]), 0.0)
    new_sum = jnp.sum(terms, axis=-1)
    product = jnp.einsum(
        "hqk,khd->hqd", terms.astype(jnp.bfloat16), value_piece, preferred_element_type=jnp.float32
    )
    return (new_max, new_sum, product)


def body(
    tokens,
    fine_gain,
    fine_query,
    fine_keyval,
    fine_out,
    down_weight,
    coarse_gain,
    coarse_query,
    coarse_keyval,
    coarse_out,
    up_weight,
):
    tok_rows = tokens.shape[0]
    width = tokens.shape[1]
    fine_heads = width // HEAD
    scale = 1.0 / math.sqrt(HEAD)
    start_row = lax.axis_index(("seq", "tp")) * tok_rows
    inputs = tokens.astype(jnp.float32)
    normed = normalize(inputs, fine_gain).astype(jnp.bfloat16)
    queries = jnp.dot(normed, fine_query, preferred_element_type=jnp.float32).astype(jnp.bfloat16)
    keyvals = jnp.dot(normed, fine_keyval, preferred_element_type=jnp.float32).astype(jnp.bfloat16)
    earlier = from_behind(keyvals, ("seq", "tp"), 1)
    key_rows = jnp.concatenate([earlier, keyvals], 0)
    span = key_rows.shape[0]
    key_heads = key_rows[:, :width].reshape(span, fine_heads, HEAD)
    value_heads = key_rows[:, width:].reshape(span, fine_heads, HEAD)
    query_heads = queries.reshape(tok_rows, fine_heads, HEAD)
    scores = (
        jnp.einsum("qhd,khd->hqk", query_heads, key_heads, preferred_element_type=jnp.float32)
        * scale
    )
    row_index = jnp.arange(tok_rows, dtype=jnp.int32)[:, None]
    col_index = jnp.arange(span, dtype=jnp.int32)[None, :]
    offset = row_index + WINDOW - col_index
    allowed = (offset >= 0) & (offset < WINDOW) & (start_row - WINDOW + col_index >= 0)
    scores = jnp.where(allowed[None], scores, big_negative)
    peak = jnp.max(scores, axis=-1, keepdims=True)
    terms = jnp.where(allowed[None], jnp.exp(scores - peak), 0.0)
    denom = jnp.sum(terms, axis=-1)
    mixed = jnp.einsum(
        "hqk,khd->qhd", terms.astype(jnp.bfloat16), value_heads, preferred_element_type=jnp.float32
    )
    local = (mixed / jnp.transpose(denom)[..., None]).reshape(tok_rows, width).astype(jnp.bfloat16)
    fine_state = (inputs + jnp.dot(local, fine_out, preferred_element_type=jnp.float32)).astype(
        jnp.bfloat16
    )
    pooled = jnp.mean(
        fine_state.astype(jnp.float32).reshape(tok_rows // SHORT, SHORT, width), axis=1
    ).astype(jnp.bfloat16)
    pooled_all = lax.all_gather(pooled, "tp", axis=0, tiled=True)
    short_cols = jnp.dot(pooled_all, down_weight, preferred_element_type=jnp.float32).astype(
        jnp.bfloat16
    )
    shortened = lax.all_gather(short_cols, "tp", axis=1, tiled=True)
    coarse_normed = normalize(shortened.astype(jnp.float32), coarse_gain).astype(jnp.bfloat16)
    coarse_rows = coarse_normed.shape[0]
    local_cols = coarse_query.shape[1]
    local_heads = local_cols // HEAD
    query_rows = lax.all_gather(coarse_query, "seq", axis=0, tiled=True)
    keyval_rows = lax.all_gather(coarse_keyval, "seq", axis=0, tiled=True)
    count = query_rows.shape[0]
    query_sum = jnp.dot(coarse_normed, query_rows, preferred_element_type=jnp.float32)
    keyval_sum = jnp.dot(
        coarse_normed,
        keyval_rows.reshape(count, 2 * local_cols),
        preferred_element_type=jnp.float32,
    )
    coarse_queries = query_sum.astype(jnp.bfloat16).reshape(coarse_rows, local_heads, HEAD)
    coarse_kv = keyval_sum.astype(jnp.bfloat16).reshape(coarse_rows, 2, local_cols)
    my_first = lax.axis_index("seq") * coarse_rows
    query_index = my_first + jnp.arange(coarse_rows, dtype=jnp.int32)
    initial = (
        jnp.full((local_heads, coarse_rows), big_negative, jnp.float32),
        jnp.zeros((local_heads, coarse_rows), jnp.float32),
        jnp.zeros((local_heads, coarse_rows, HEAD), jnp.float32),
    )
    piece = lax.all_gather(coarse_kv, "seq", axis=0, tiled=True)
    count = piece.shape[0]
    key_piece = piece[:, 0].reshape(count, local_heads, HEAD)
    value_piece = piece[:, 1].reshape(count, local_heads, HEAD)
    final = lax.cond(
        jnp.int32(0) < my_first + coarse_rows,
        lambda: online_update(initial, coarse_queries, key_piece, value_piece, query_index),
        lambda: initial,
    )
    head_out = final[2] / final[1][..., None]
    coarse_heads = (
        jnp.transpose(head_out, (1, 0, 2)).reshape(coarse_rows, local_cols).astype(jnp.bfloat16)
    )
    partials = jnp.dot(coarse_heads, coarse_out, preferred_element_type=jnp.float32)
    attended = lax.psum_scatter(
        partials.astype(jnp.bfloat16), "tp", scatter_dimension=1, tiled=True
    ).astype(jnp.float32)
    coarse_state = (short_cols.astype(jnp.float32) + attended).astype(jnp.bfloat16)
    prior_row = from_behind(coarse_state[coarse_rows - 1 :], "seq", 1)
    delayed = jnp.concatenate([prior_row, coarse_state[: coarse_rows - 1]], 0)
    lifted = lax.psum_scatter(
        jnp.dot(delayed, up_weight, preferred_element_type=jnp.float32).astype(jnp.bfloat16),
        "tp",
        scatter_dimension=0,
        tiled=True,
    ).astype(jnp.float32)
    result = fine_state.astype(jnp.float32) + jnp.repeat(lifted, SHORT, axis=0)
    return result.astype(jnp.bfloat16)


def flip(index, bit):
    return index + bit - 2 * bit * lax.rem(lax.div(index, jnp.int32(bit)), jnp.int32(2))


def bits_of(size):
    out, bit = [], size // 2
    while bit:
        out.append(bit)
        bit //= 2
    return out


def dot32(left, right):
    return jnp.dot(left, right, preferred_element_type=jnp.float32)


def dot_t(left, right):
    return lax.dot_general(
        left, right, (((1,), (1,)), ((), ())), preferred_element_type=jnp.float32
    )


def section_kernel(
    seq, tp,
    tokens, fine_gain, fine_query, fine_keyval, fine_out, down_weight, coarse_gain, coarse_query,
    coarse_kv, coarse_out, up_weight,
    result,
    both, wq, wkv, wo, down_all, weights, wout, wup,
    normed, queries, key_rows, local, fine_state, pooled_all, coarse_normed, projected, sums,
    heads_out, heads_in, coarse_heads, short_cols, send1, recv1, state, prior, send2, recv2,
    load_sem, halo_s, halo_r, w_s, w_r, d_s, d_r, p_s, p_r, h_s, h_r, r1_s, r1_r, row_s, row_r,
    r2_s, r2_r,
):
    me_s = lax.axis_index("seq")
    me_t = lax.axis_index("tp")
    rows, width = tokens.shape
    scale = 1.0 / math.sqrt(HEAD)
    total = seq * tp
    lin = me_s * tp + me_t
    after = lax.rem(lin + 1, total)
    before = lax.rem(lin + total - 1, total)

    def around(index, step, size):
        return lax.rem(index + step, size)

    def remote(src, dst, send, recv, device):
        copy = pltpu.make_async_remote_copy(
            src_ref=src, dst_ref=dst, send_sem=send, recv_sem=recv,
            device_id=device, device_id_type=pl.DeviceIdType.MESH,
        )
        copy.start()
        return copy

    def load(src, dst, index):
        copy = pltpu.make_async_copy(src, dst, load_sem.at[index])
        copy.start()
        return copy

    def linear(index):
        return {"seq": lax.div(index, tp), "tp": lax.rem(index, tp)}

    barrier = pltpu.get_barrier_semaphore()
    peers = [{"seq": around(me_s, d, seq)} for d in range(1, seq)]
    peers += [{"tp": around(me_t, d, tp)} for d in range(1, tp)]
    peers += [linear(after), linear(before)]
    in_tokens = load(tokens, both.at[pl.ds(rows, rows)], 0)
    in_wkv = load(fine_keyval, wkv, 1)
    in_wq = load(fine_query, wq, 2)
    in_wo = load(fine_out, wo, 3)
    in_down = load(down_weight, down_all.at[me_t], 4)
    own = coarse_query.shape[1] // seq

    def head_parts(dest):
        cols = pl.ds(pl.multiple_of(dest * own, own), own)
        sources = [coarse_query.at[:, cols], coarse_kv.at[0, :, cols], coarse_kv.at[1, :, cols]]
        return [(part, weights.at[me_s, :, pl.ds(k * own, own)]) for k, part in enumerate(sources)]

    in_w = [load(src, dst, 8 + k) for k, (src, dst) in enumerate(head_parts(me_s))]
    in_wout = load(coarse_out, wout, 6)
    in_wup = load(up_weight, wup, 7)
    for peer in peers:
        pl.semaphore_signal(barrier, inc=1, device_id=peer, device_id_type=pl.DeviceIdType.MESH)
    pl.semaphore_wait(barrier, len(peers))

    halo = remote(tokens, both.at[pl.ds(0, rows)], halo_s, halo_r, linear(after))
    order = sorted(range(1, seq), key=lambda d: abs(2 * d - seq))
    w_copies = {}

    def send_weights(offsets):
        for d in offsets:
            dest = around(me_s, d, seq)
            w_copies[d] = [
                remote(
                    src, dst, w_s.at[3 * (d - 1) + k], w_r.at[3 * (d - 1) + k], {"seq": dest}
                )
                for k, (src, dst) in enumerate(head_parts(dest))
            ]

    early = (seq + 1) // 4
    send_weights(order[:early])
    tp_bits = bits_of(tp)
    gain = fine_gain[...]

    def norm_rows(first):
        values = both[pl.ds(first, rows), :].astype(jnp.float32)
        normed[pl.ds(first, rows), :] = normalize(values, gain).astype(jnp.bfloat16)

    in_tokens.wait()
    norm_rows(rows)
    in_wq.wait()
    tile = 2 * HEAD

    @pl.loop(0, width // tile)
    def _(i):
        cols = pl.ds(pl.multiple_of(i * tile, tile), tile)
        queries[:, cols] = dot32(normed[rows:, :], wq[:, cols]).astype(jnp.bfloat16)

    in_wkv.wait()

    def project_rows(first):
        @pl.loop(0, 2 * width // tile)
        def _(i):
            cols = pl.ds(pl.multiple_of(i * tile, tile), tile)
            key_rows[pl.ds(first, rows), cols] = dot32(
                normed[pl.ds(first, rows), :], wkv[:, cols]
            ).astype(jnp.bfloat16)

    project_rows(rows)
    d_first = [
        remote(
            down_weight, down_all.at[me_t], d_s.at[bit - 1], d_r.at[bit - 1],
            {"tp": flip(me_t, bit)},
        )
        for bit in tp_bits
    ]
    halo.wait()
    norm_rows(0)
    project_rows(0)

    row_index = lax.broadcasted_iota(jnp.int32, (rows, 2 * rows), 0)
    col_index = lax.broadcasted_iota(jnp.int32, (rows, 2 * rows), 1)
    offset = row_index + rows - col_index
    allowed = (offset >= 0) & (offset < WINDOW) & (lin * rows - rows + col_index >= 0)

    def attend(query, key, value, mask):
        scores = jnp.where(mask, dot_t(query, key) * scale, big_negative)
        peak = jnp.max(scores, axis=-1, keepdims=True)
        terms = jnp.where(mask, jnp.exp(scores - peak), 0.0)
        denom = jnp.sum(terms, axis=-1, keepdims=True)
        return (dot32(terms.astype(jnp.bfloat16), value) / denom).astype(jnp.bfloat16)

    @pl.loop(0, width // HEAD)
    def _(h):
        cols = pl.ds(pl.multiple_of(h * HEAD, HEAD), HEAD)
        vcols = pl.ds(pl.multiple_of(width + h * HEAD, HEAD), HEAD)
        local[:, cols] = attend(queries[:, cols], key_rows[:, cols], key_rows[:, vcols], allowed)

    in_wo.wait()
    pool_rows = rows // SHORT

    @pl.loop(0, width // tile)
    def _(i):
        cols = pl.ds(pl.multiple_of(i * tile, tile), tile)
        value = both[rows:, cols].astype(jnp.float32) + dot32(local[...], wo[:, cols])
        value = value.astype(jnp.bfloat16)
        fine_state[:, cols] = value
        mean = jnp.mean(value.astype(jnp.float32).reshape(pool_rows, SHORT, tile), axis=1)
        pooled_all[lin, :, cols] = mean.astype(jnp.bfloat16)

    done = []
    held = [lin]
    count = 0
    for axis, bits in (("seq", bits_of(seq)), ("tp", tp_bits)):
        for bit in bits:
            stride = bit * tp if axis == "seq" else bit
            where = {axis: flip(me_s if axis == "seq" else me_t, bit)}
            copies = []
            for slot in held:
                copies.append(
                    remote(
                        pooled_all.at[slot], pooled_all.at[slot], p_s.at[count], p_r.at[count],
                        where,
                    )
                )
                count += 1
            if axis == "seq" and bit == bits[-1]:
                send_weights(order[early:])
            for copy in copies:
                copy.wait_recv()
            done += copies
            held = held + [flip(slot, stride) for slot in held]
    d_done = list(d_first)
    for copy in d_first[:1]:
        copy.wait_recv()
    have = [tp_bits[0]]
    index = tp - 1
    extra = []
    for k, bit in enumerate(tp_bits[1:]):
        subs = list(have)
        now = []
        for sub in subs:
            slot = me_t
            for other in tp_bits:
                if sub & other:
                    slot = flip(slot, other)
            number = bit + sub - 1
            now.append(
                remote(
                    down_all.at[slot], down_all.at[slot], d_s.at[number], d_r.at[number],
                    {"tp": flip(me_t, bit)},
                )
            )
        d_first[k + 1].wait_recv()
        for copy in now:
            copy.wait_recv()
        extra += now
        have = have + [bit] + [bit + sub for sub in subs]
    in_down.wait()

    per = seq // 2 if seq > 1 else 1
    crows = pool_rows * tp
    block = 2 * crows
    cgain = coarse_gain[...]

    @pl.loop(0, seq // 2)
    def _(i):
        first = pl.multiple_of(i * block, block)
        pooled = pooled_all[pl.ds(i * 2 * tp, 2 * tp)].reshape(block, width)
        total_sq = jnp.zeros((block, 1), jnp.float32)
        fcols = down_all.shape[2]
        half = fcols // 2
        for t in range(tp):
            for u in range(2):
                part = dot32(pooled, down_all[t, :, u * half : (u + 1) * half]).astype(jnp.bfloat16)
                wide = part.astype(jnp.float32)
                total_sq += jnp.sum(wide * wide, axis=-1, keepdims=True)
                base = t * fcols + u * half
                coarse_normed[pl.ds(first, block), base : base + half] = part
        factor = lax.rsqrt(total_sq / (tp * fcols) + epsilon)
        for t in range(2 * tp):
            cols = slice(t * half, (t + 1) * half)
            wide = coarse_normed[pl.ds(first, block), cols].astype(jnp.float32)
            coarse_normed[pl.ds(first, block), cols] = (wide * factor * cgain[:, cols]).astype(
                jnp.bfloat16
            )

    mine = pooled_all[pl.ds(me_s * tp, tp)].reshape(crows, width)
    fcols = down_all.shape[2]
    for u in range(2):
        cols = slice(u * fcols // 2, (u + 1) * fcols // 2)
        short_cols[:, cols] = dot32(mine, down_all[me_t, :, cols])
    depth, three = weights.shape[1:]

    for d in [0] + order:
        for copy in w_copies[d] if d else in_w:
            copy.wait_recv() if d else copy.wait()
        source = around(me_s, seq - d, seq)

        @pl.loop(0, seq // 2)
        def _(i, d=d, source=source):
            at = pl.ds(pl.multiple_of(i * block, block), block)
            cols = pl.ds(pl.multiple_of(source * depth, depth), depth)
            product = dot32(coarse_normed[at, cols], weights[source])
            if d == order[-1]:
                projected[at, :] = (sums[at, :] + product).astype(jnp.bfloat16)
            elif d:
                sums[at, :] += product
            else:
                sums[at, :] = product

    for i in range(seq // 2):
        extent = (i + 1) * block
        r = lax.broadcasted_iota(jnp.int32, (block, extent), 0) + i * block
        c = lax.broadcasted_iota(jnp.int32, (block, extent), 1)
        for h in range(own // HEAD):
            part = slice(h * HEAD, (h + 1) * HEAD)
            kpart = slice(own + h * HEAD, own + (h + 1) * HEAD)
            vpart = slice(2 * own + h * HEAD, 2 * own + (h + 1) * HEAD)
            out = attend(
                projected[i * block : extent, part], projected[:extent, kpart],
                projected[:extent, vpart], c <= r,
            )
            heads_out[2 * i : 2 * i + 2, :, part] = out.reshape(2, crows, HEAD)

    heads_in[me_s] = heads_out[me_s]
    h_copies = []
    for d in order:
        dest = around(me_s, d, seq)
        h_copies.append(
            remote(
                heads_out.at[dest], heads_in.at[me_s], h_s.at[d - 1], h_r.at[d - 1],
                {"seq": dest},
            )
        )
    in_wout.wait()
    in_wup.wait()
    for copy in h_copies:
        copy.wait_recv()
    for j in range(seq):
        coarse_heads[:, j * own : (j + 1) * own] = heads_in[j]

    def partial(t, store):
        @pl.loop(0, fcols // tile)
        def _(i):
            cols = pl.ds(pl.multiple_of(i * tile, tile), tile)
            wcols = pl.ds(pl.multiple_of(t * fcols + i * tile, tile), tile)
            store(cols, dot32(coarse_heads[...], wout[:, wcols]))

    tp_order = sorted(range(1, tp), key=lambda d: abs(2 * d - tp))
    r1 = []
    for d in tp_order:
        dest = around(me_t, d, tp)

        def put(cols, value, d=d):
            send1[d - 1, :, cols] = value.astype(jnp.bfloat16)

        partial(dest, put)
        r1.append(
            remote(
                send1.at[d - 1], recv1.at[d - 1], r1_s.at[d - 1], r1_r.at[d - 1], {"tp": dest}
            )
        )

    def keep(cols, value):
        short_cols[:, cols] = short_cols[:, cols].astype(jnp.bfloat16).astype(jnp.float32) + value

    partial(me_t, keep)
    for copy in r1:
        copy.wait_recv()
    whole = short_cols[...]
    for d in range(1, tp):
        whole += recv1[d - 1].astype(jnp.float32)
    state[...] = whole.astype(jnp.bfloat16)
    slab = prior.shape[0]
    row_copy = remote(
        state.at[pl.ds(crows - slab, slab)], prior, row_s, row_r, {"seq": around(me_s, 1, seq)}
    )
    rolled = pltpu.roll(state[...].astype(jnp.float32), 1, 0)
    row_copy.wait_recv()
    previous = prior[...].astype(jnp.float32)[slab - 1 : slab, :]
    previous = jnp.where(me_s > 0, previous, 0.0)
    top = lax.broadcasted_iota(jnp.int32, rolled.shape, 0) == 0
    delayed = jnp.where(top, previous, rolled).astype(jnp.bfloat16)
    coarse_heads[...] = delayed

    @pl.loop(0, width // tile)
    def _(i):
        cols = pl.ds(pl.multiple_of(i * tile, tile), tile)
        short_cols[:, cols] = dot32(coarse_heads[...], wup[:, cols])

    r2 = []
    for d in tp_order:
        dest = around(me_t, d, tp)
        part = short_cols[pl.ds(pl.multiple_of(dest * pool_rows, pool_rows), pool_rows), :]
        send2[d - 1] = part.astype(jnp.bfloat16)
        r2.append(
            remote(
                send2.at[d - 1], recv2.at[d - 1], r2_s.at[d - 1], r2_r.at[d - 1], {"tp": dest}
            )
        )
    lifted = short_cols[pl.ds(pl.multiple_of(me_t * pool_rows, pool_rows), pool_rows), :]
    for copy in r2:
        copy.wait_recv()
    for d in range(1, tp):
        lifted += recv2[d - 1].astype(jnp.float32)
    spread = jnp.broadcast_to(lifted[:, None, :], (pool_rows, SHORT, width)).reshape(rows, width)
    result[...] = (fine_state[...].astype(jnp.float32) + spread).astype(jnp.bfloat16)
    w_flat = [copy for group in w_copies.values() for copy in group]
    for copy in w_flat + d_done + extra + done + h_copies + r1 + [row_copy] + r2:
        copy.wait_send()


def head_body(
    tokens,
    fine_gain,
    fine_query,
    fine_keyval,
    fine_out,
    down_weight,
    coarse_gain,
    coarse_query,
    coarse_keyval,
    coarse_out,
    up_weight,
):
    seq, tp = lax.axis_size("seq"), lax.axis_size("tp")
    rows, width = tokens.shape
    depth, local_cols = coarse_query.shape
    own = local_cols // seq
    pool_rows = rows // SHORT
    crows = pool_rows * tp
    count = crows * seq
    bf, f32 = jnp.bfloat16, jnp.float32
    V = pltpu.VMEM
    dma = lambda n: pltpu.SemaphoreType.DMA((n,))
    one = pltpu.SemaphoreType.DMA
    anywhere = pl.BlockSpec(memory_space=pl.ANY)
    vmem = pl.BlockSpec(memory_space=pltpu.VMEM)
    return pl.pallas_call(
        functools.partial(section_kernel, seq, tp),
        out_shape=jax.ShapeDtypeStruct((rows, width), bf),
        in_specs=[anywhere, vmem, anywhere, anywhere, anywhere, anywhere, vmem, anywhere,
                  anywhere, anywhere, anywhere],
        out_specs=vmem,
        scratch_shapes=[
            V((2 * rows, width), bf), V(fine_query.shape, bf), V(fine_keyval.shape, bf),
            V(fine_out.shape, bf), V((tp,) + down_weight.shape, bf), V((seq, depth, 3 * own), bf),
            V(coarse_out.shape, bf), V(up_weight.shape, bf),
            V((2 * rows, width), bf), V((rows, width), bf), V((2 * rows, 2 * width), bf),
            V((rows, width), bf), V((rows, width), bf), V((seq * tp, pool_rows, width), bf),
            V((count, tp * local_cols), bf), V((count, 3 * own), bf), V((count, 3 * own), f32),
            V((seq, crows, own), bf), V((seq, crows, own), bf), V((crows, local_cols), bf),
            V((crows, local_cols), f32), V((tp - 1, crows, local_cols), bf),
            V((tp - 1, crows, local_cols), bf), V((crows, local_cols), bf), V((16, local_cols), bf),
            V((tp - 1, pool_rows, width), bf), V((tp - 1, pool_rows, width), bf),
            dma(11), one(()), one(()), dma(3 * (seq - 1)), dma(3 * (seq - 1)), dma(tp - 1), dma(tp - 1),
            dma(seq * tp - 1), dma(seq * tp - 1), dma(seq - 1), dma(seq - 1),
            dma(tp - 1), dma(tp - 1), one(()), one(()), dma(tp - 1), dma(tp - 1),
        ],
        compiler_params=pltpu.CompilerParams(
            collective_id=0, has_side_effects=True, vmem_limit_bytes=62 * 1024 * 1024
        ),
    )(tokens, fine_gain[None], fine_query, fine_keyval, fine_out, down_weight, coarse_gain[None],
      coarse_query, jnp.transpose(coarse_keyval, (1, 0, 2)), coarse_out, up_weight)


def chosen(*args):
    seq, tp = lax.axis_size("seq"), lax.axis_size("tp")
    local_heads = args[7].shape[1] // HEAD
    powers = seq & (seq - 1) == 0 and tp & (tp - 1) == 0 and seq > 1 and tp > 1
    square = args[10].shape[0] == args[10].shape[1] == args[7].shape[1]
    if local_heads % seq == 0 and args[0].shape[0] == WINDOW and powers and square:
        return head_body(*args)
    return body(*args)


def solution(mesh):
    return jax.shard_map(
        chosen,
        mesh=mesh,
        in_specs=(
            P(("seq", "tp"), None),
            P(),
            P(),
            P(),
            P(),
            P(None, "tp"),
            P(),
            P("seq", "tp"),
            P("seq", None, "tp"),
            P("tp", None),
            P("tp", None),
        ),
        out_specs=P(("seq", "tp"), None),
        check_vma=False,
    )
```

```python
import functools
import math

import jax
import jax.numpy as jnp
from jax import lax
from jax.experimental import pallas as pl
from jax.experimental.pallas import tpu as pltpu
from jax.sharding import PartitionSpec as P

HEAD = 128
WINDOW = 256
SHORT = 8


epsilon = 1e-06
big_negative = -1e30


def from_behind(array, axis, by):
    size = lax.axis_size(axis)
    pairs = [(i, i + by) for i in range(size) if 0 <= i + by < size]
    return lax.ppermute(array, axis, pairs)


def normalize(values, scale_gain):
    mean_square = jnp.mean(values * values, axis=-1, keepdims=True)
    return values * lax.rsqrt(mean_square + epsilon) * scale_gain


def online_update(state, query_heads, key_piece, value_piece, query_index):
    running_max, running_sum, accumulate = state
    scale = 1.0 / math.sqrt(HEAD)
    scores = (
        jnp.einsum("qhd,khd->hqk", query_heads, key_piece, preferred_element_type=jnp.float32)
        * scale
    )
    key_index = jnp.arange(key_piece.shape[0], dtype=jnp.int32)
    allowed = key_index[None, :] <= query_index[:, None]
    scores = jnp.where(allowed[None], scores, big_negative)
    new_max = jnp.maximum(running_max, jnp.max(scores, axis=-1))
    terms = jnp.where(allowed[None], jnp.exp(scores - new_max[..., None]), 0.0)
    new_sum = jnp.sum(terms, axis=-1)
    product = jnp.einsum(
        "hqk,khd->hqd", terms.astype(jnp.bfloat16), value_piece, preferred_element_type=jnp.float32
    )
    return (new_max, new_sum, product)


def body(
    tokens,
    fine_gain,
    fine_query,
    fine_keyval,
    fine_out,
    down_weight,
    coarse_gain,
    coarse_query,
    coarse_keyval,
    coarse_out,
    up_weight,
):
    tok_rows = tokens.shape[0]
    width = tokens.shape[1]
    fine_heads = width // HEAD
    scale = 1.0 / math.sqrt(HEAD)
    start_row = lax.axis_index(("seq", "tp")) * tok_rows
    inputs = tokens.astype(jnp.float32)
    normed = normalize(inputs, fine_gain).astype(jnp.bfloat16)
    queries = jnp.dot(normed, fine_query, preferred_element_type=jnp.float32).astype(jnp.bfloat16)
    keyvals = jnp.dot(normed, fine_keyval, preferred_element_type=jnp.float32).astype(jnp.bfloat16)
    earlier = from_behind(keyvals, ("seq", "tp"), 1)
    key_rows = jnp.concatenate([earlier, keyvals], 0)
    span = key_rows.shape[0]
    key_heads = key_rows[:, :width].reshape(span, fine_heads, HEAD)
    value_heads = key_rows[:, width:].reshape(span, fine_heads, HEAD)
    query_heads = queries.reshape(tok_rows, fine_heads, HEAD)
    scores = (
        jnp.einsum("qhd,khd->hqk", query_heads, key_heads, preferred_element_type=jnp.float32)
        * scale
    )
    row_index = jnp.arange(tok_rows, dtype=jnp.int32)[:, None]
    col_index = jnp.arange(span, dtype=jnp.int32)[None, :]
    offset = row_index + WINDOW - col_index
    allowed = (offset >= 0) & (offset < WINDOW) & (start_row - WINDOW + col_index >= 0)
    scores = jnp.where(allowed[None], scores, big_negative)
    peak = jnp.max(scores, axis=-1, keepdims=True)
    terms = jnp.where(allowed[None], jnp.exp(scores - peak), 0.0)
    denom = jnp.sum(terms, axis=-1)
    mixed = jnp.einsum(
        "hqk,khd->qhd", terms.astype(jnp.bfloat16), value_heads, preferred_element_type=jnp.float32
    )
    local = (mixed / jnp.transpose(denom)[..., None]).reshape(tok_rows, width).astype(jnp.bfloat16)
    fine_state = (inputs + jnp.dot(local, fine_out, preferred_element_type=jnp.float32)).astype(
        jnp.bfloat16
    )
    pooled = jnp.mean(
        fine_state.astype(jnp.float32).reshape(tok_rows // SHORT, SHORT, width), axis=1
    ).astype(jnp.bfloat16)
    pooled_all = lax.all_gather(pooled, "tp", axis=0, tiled=True)
    short_cols = jnp.dot(pooled_all, down_weight, preferred_element_type=jnp.float32).astype(
        jnp.bfloat16
    )
    shortened = lax.all_gather(short_cols, "tp", axis=1, tiled=True)
    coarse_normed = normalize(shortened.astype(jnp.float32), coarse_gain).astype(jnp.bfloat16)
    coarse_rows = coarse_normed.shape[0]
    local_cols = coarse_query.shape[1]
    local_heads = local_cols // HEAD
    query_rows = lax.all_gather(coarse_query, "seq", axis=0, tiled=True)
    keyval_rows = lax.all_gather(coarse_keyval, "seq", axis=0, tiled=True)
    count = query_rows.shape[0]
    query_sum = jnp.dot(coarse_normed, query_rows, preferred_element_type=jnp.float32)
    keyval_sum = jnp.dot(
        coarse_normed,
        keyval_rows.reshape(count, 2 * local_cols),
        preferred_element_type=jnp.float32,
    )
    coarse_queries = query_sum.astype(jnp.bfloat16).reshape(coarse_rows, local_heads, HEAD)
    coarse_kv = keyval_sum.astype(jnp.bfloat16).reshape(coarse_rows, 2, local_cols)
    my_first = lax.axis_index("seq") * coarse_rows
    query_index = my_first + jnp.arange(coarse_rows, dtype=jnp.int32)
    initial = (
        jnp.full((local_heads, coarse_rows), big_negative, jnp.float32),
        jnp.zeros((local_heads, coarse_rows), jnp.float32),
        jnp.zeros((local_heads, coarse_rows, HEAD), jnp.float32),
    )
    piece = lax.all_gather(coarse_kv, "seq", axis=0, tiled=True)
    count = piece.shape[0]
    key_piece = piece[:, 0].reshape(count, local_heads, HEAD)
    value_piece = piece[:, 1].reshape(count, local_heads, HEAD)
    final = lax.cond(
        jnp.int32(0) < my_first + coarse_rows,
        lambda: online_update(initial, coarse_queries, key_piece, value_piece, query_index),
        lambda: initial,
    )
    head_out = final[2] / final[1][..., None]
    coarse_heads = (
        jnp.transpose(head_out, (1, 0, 2)).reshape(coarse_rows, local_cols).astype(jnp.bfloat16)
    )
    partials = jnp.dot(coarse_heads, coarse_out, preferred_element_type=jnp.float32)
    attended = lax.psum_scatter(
        partials.astype(jnp.bfloat16), "tp", scatter_dimension=1, tiled=True
    ).astype(jnp.float32)
    coarse_state = (short_cols.astype(jnp.float32) + attended).astype(jnp.bfloat16)
    prior_row = from_behind(coarse_state[coarse_rows - 1 :], "seq", 1)
    delayed = jnp.concatenate([prior_row, coarse_state[: coarse_rows - 1]], 0)
    lifted = lax.psum_scatter(
        jnp.dot(delayed, up_weight, preferred_element_type=jnp.float32).astype(jnp.bfloat16),
        "tp",
        scatter_dimension=0,
        tiled=True,
    ).astype(jnp.float32)
    result = fine_state.astype(jnp.float32) + jnp.repeat(lifted, SHORT, axis=0)
    return result.astype(jnp.bfloat16)


def flip(index, bit):
    return index + bit - 2 * bit * lax.rem(lax.div(index, jnp.int32(bit)), jnp.int32(2))


def bits_of(size):
    out, bit = [], size // 2
    while bit:
        out.append(bit)
        bit //= 2
    return out


def dot32(left, right):
    return jnp.dot(left, right, preferred_element_type=jnp.float32)


def dot_t(left, right):
    return lax.dot_general(
        left, right, (((1,), (1,)), ((), ())), preferred_element_type=jnp.float32
    )


def section_kernel(
    seq, tp,
    tokens, fine_gain, fine_query, fine_keyval, fine_out, down_weight, coarse_gain, coarse_query,
    coarse_kv, coarse_out, up_weight,
    result,
    both, wq, wkv, wo, down_all, weights, wout, wup,
    normed, queries, key_rows, local, fine_state, pooled_all, coarse_normed, projected, sums,
    heads_out, heads_in, coarse_heads, short_cols, send1, recv1, state, prior, send2, recv2,
    load_sem, halo_s, halo_r, w_s, w_r, d_s, d_r, p_s, p_r, h_s, h_r, r1_s, r1_r, row_s, row_r,
    r2_s, r2_r,
):
    me_s = lax.axis_index("seq")
    me_t = lax.axis_index("tp")
    rows, width = tokens.shape
    scale = 1.0 / math.sqrt(HEAD)
    total = seq * tp
    lin = me_s * tp + me_t
    after = lax.rem(lin + 1, total)
    before = lax.rem(lin + total - 1, total)

    def around(index, step, size):
        return lax.rem(index + step, size)

    def remote(src, dst, send, recv, device):
        copy = pltpu.make_async_remote_copy(
            src_ref=src, dst_ref=dst, send_sem=send, recv_sem=recv,
            device_id=device, device_id_type=pl.DeviceIdType.MESH,
        )
        copy.start()
        return copy

    def load(src, dst, index):
        copy = pltpu.make_async_copy(src, dst, load_sem.at[index])
        copy.start()
        return copy

    def linear(index):
        return {"seq": lax.div(index, tp), "tp": lax.rem(index, tp)}

    barrier = pltpu.get_barrier_semaphore()
    peers = [{"seq": around(me_s, d, seq)} for d in range(1, seq)]
    peers += [{"tp": around(me_t, d, tp)} for d in range(1, tp)]
    peers += [linear(after), linear(before)]
    in_tokens = load(tokens, both.at[pl.ds(rows, rows)], 0)
    in_wkv = load(fine_keyval, wkv, 1)
    in_wq = load(fine_query, wq, 2)
    in_wo = load(fine_out, wo, 3)
    in_down = load(down_weight, down_all.at[me_t], 4)
    own = coarse_query.shape[1] // seq

    def head_parts(dest):
        cols = pl.ds(pl.multiple_of(dest * own, own), own)
        sources = [coarse_query.at[:, cols], coarse_kv.at[0, :, cols], coarse_kv.at[1, :, cols]]
        return [(part, weights.at[me_s, :, pl.ds(k * own, own)]) for k, part in enumerate(sources)]

    in_w = [load(src, dst, 8 + k) for k, (src, dst) in enumerate(head_parts(me_s))]
    in_wout = load(coarse_out, wout, 6)
    in_wup = load(up_weight, wup, 7)
    for peer in peers:
        pl.semaphore_signal(barrier, inc=1, device_id=peer, device_id_type=pl.DeviceIdType.MESH)
    pl.semaphore_wait(barrier, len(peers))

    halo = remote(tokens, both.at[pl.ds(0, rows)], halo_s, halo_r, linear(after))
    order = sorted(range(1, seq), key=lambda d: abs(2 * d - seq))
    w_copies = {}

    def send_weights(offsets):
        for d in offsets:
            dest = around(me_s, d, seq)
            w_copies[d] = [
                remote(
                    src, dst, w_s.at[3 * (d - 1) + k], w_r.at[3 * (d - 1) + k], {"seq": dest}
                )
                for k, (src, dst) in enumerate(head_parts(dest))
            ]

    early = (seq + 1) // 4
    send_weights(order[:early])
    tp_bits = bits_of(tp)
    gain = fine_gain[...]

    def norm_rows(first):
        values = both[pl.ds(first, rows), :].astype(jnp.float32)
        normed[pl.ds(first, rows), :] = normalize(values, gain).astype(jnp.bfloat16)

    in_tokens.wait()
    norm_rows(rows)
    in_wq.wait()
    tile = 2 * HEAD

    @pl.loop(0, width // tile)
    def _(i):
        cols = pl.ds(pl.multiple_of(i * tile, tile), tile)
        queries[:, cols] = dot32(normed[rows:, :], wq[:, cols]).astype(jnp.bfloat16)

    in_wkv.wait()

    def project_rows(first):
        @pl.loop(0, 2 * width // tile)
        def _(i):
            cols = pl.ds(pl.multiple_of(i * tile, tile), tile)
            key_rows[pl.ds(first, rows), cols] = dot32(
                normed[pl.ds(first, rows), :], wkv[:, cols]
            ).astype(jnp.bfloat16)

    project_rows(rows)
    d_first = [
        remote(
            down_weight, down_all.at[me_t], d_s.at[bit - 1], d_r.at[bit - 1],
            {"tp": flip(me_t, bit)},
        )
        for bit in tp_bits
    ]
    halo.wait()
    norm_rows(0)
    project_rows(0)

    row_index = lax.broadcasted_iota(jnp.int32, (rows, 2 * rows), 0)
    col_index = lax.broadcasted_iota(jnp.int32, (rows, 2 * rows), 1)
    offset = row_index + rows - col_index
    allowed = (offset >= 0) & (offset < WINDOW) & (lin * rows - rows + col_index >= 0)

    def attend(query, key, value, mask):
        scores = jnp.where(mask, dot_t(query, key) * scale, big_negative)
        peak = jnp.max(scores, axis=-1, keepdims=True)
        terms = jnp.where(mask, jnp.exp(scores - peak), 0.0)
        denom = jnp.sum(terms, axis=-1, keepdims=True)
        return (dot32(terms.astype(jnp.bfloat16), value) / denom).astype(jnp.bfloat16)

    @pl.loop(0, width // HEAD)
    def _(h):
        cols = pl.ds(pl.multiple_of(h * HEAD, HEAD), HEAD)
        vcols = pl.ds(pl.multiple_of(width + h * HEAD, HEAD), HEAD)
        local[:, cols] = attend(queries[:, cols], key_rows[:, cols], key_rows[:, vcols], allowed)

    in_wo.wait()
    pool_rows = rows // SHORT

    @pl.loop(0, width // tile)
    def _(i):
        cols = pl.ds(pl.multiple_of(i * tile, tile), tile)
        value = both[rows:, cols].astype(jnp.float32) + dot32(local[...], wo[:, cols])
        value = value.astype(jnp.bfloat16)
        fine_state[:, cols] = value
        mean = jnp.mean(value.astype(jnp.float32).reshape(pool_rows, SHORT, tile), axis=1)
        pooled_all[lin, :, cols] = mean.astype(jnp.bfloat16)

    done = []
    held = [lin]
    count = 0
    for axis, bits in (("seq", bits_of(seq)), ("tp", tp_bits)):
        for bit in bits:
            stride = bit * tp if axis == "seq" else bit
            where = {axis: flip(me_s if axis == "seq" else me_t, bit)}
            copies = []
            for slot in held:
                copies.append(
                    remote(
                        pooled_all.at[slot], pooled_all.at[slot], p_s.at[count], p_r.at[count],
                        where,
                    )
                )
                count += 1
            if axis == "seq" and bit == bits[-1]:
                send_weights(order[early:])
            for copy in copies:
                copy.wait_recv()
            done += copies
            held = held + [flip(slot, stride) for slot in held]
    d_done = list(d_first)
    for copy in d_first[:1]:
        copy.wait_recv()
    have = [tp_bits[0]]
    index = tp - 1
    extra = []
    for k, bit in enumerate(tp_bits[1:]):
        subs = list(have)
        now = []
        for sub in subs:
            slot = me_t
            for other in tp_bits:
                if sub & other:
                    slot = flip(slot, other)
            number = bit + sub - 1
            now.append(
                remote(
                    down_all.at[slot], down_all.at[slot], d_s.at[number], d_r.at[number],
                    {"tp": flip(me_t, bit)},
                )
            )
        d_first[k + 1].wait_recv()
        for copy in now:
            copy.wait_recv()
        extra += now
        have = have + [bit] + [bit + sub for sub in subs]
    in_down.wait()

    per = seq // 2 if seq > 1 else 1
    crows = pool_rows * tp
    block = 2 * crows
    cgain = coarse_gain[...]

    @pl.loop(0, seq // 2)
    def _(i):
        first = pl.multiple_of(i * block, block)
        pooled = pooled_all[pl.ds(i * 2 * tp, 2 * tp)].reshape(block, width)
        total_sq = jnp.zeros((block, 1), jnp.float32)
        fcols = down_all.shape[2]
        half = fcols // 2
        for t in range(tp):
            for u in range(2):
                part = dot32(pooled, down_all[t, :, u * half : (u + 1) * half]).astype(jnp.bfloat16)
                wide = part.astype(jnp.float32)
                total_sq += jnp.sum(wide * wide, axis=-1, keepdims=True)
                base = t * fcols + u * half
                coarse_normed[pl.ds(first, block), base : base + half] = part
        factor = lax.rsqrt(total_sq / (tp * fcols) + epsilon)
        for t in range(2 * tp):
            cols = slice(t * half, (t + 1) * half)
            wide = coarse_normed[pl.ds(first, block), cols].astype(jnp.float32)
            coarse_normed[pl.ds(first, block), cols] = (wide * factor * cgain[:, cols]).astype(
                jnp.bfloat16
            )

    mine = pooled_all[pl.ds(me_s * tp, tp)].reshape(crows, width)
    fcols = down_all.shape[2]
    for u in range(2):
        cols = slice(u * fcols // 2, (u + 1) * fcols // 2)
        short_cols[:, cols] = dot32(mine, down_all[me_t, :, cols])
    depth, three = weights.shape[1:]

    for d in [0] + order:
        for copy in w_copies[d] if d else in_w:
            copy.wait_recv() if d else copy.wait()
        source = around(me_s, seq - d, seq)

        @pl.loop(0, seq // 2)
        def _(i, d=d, source=source):
            at = pl.ds(pl.multiple_of(i * block, block), block)
            cols = pl.ds(pl.multiple_of(source * depth, depth), depth)
            product = dot32(coarse_normed[at, cols], weights[source])
            if d == order[-1]:
                projected[at, :] = (sums[at, :] + product).astype(jnp.bfloat16)
            elif d:
                sums[at, :] += product
            else:
                sums[at, :] = product

    for i in range(seq // 2):
        extent = (i + 1) * block
        r = lax.broadcasted_iota(jnp.int32, (block, extent), 0) + i * block
        c = lax.broadcasted_iota(jnp.int32, (block, extent), 1)
        for h in range(own // HEAD):
            part = slice(h * HEAD, (h + 1) * HEAD)
            kpart = slice(own + h * HEAD, own + (h + 1) * HEAD)
            vpart = slice(2 * own + h * HEAD, 2 * own + (h + 1) * HEAD)
            out = attend(
                projected[i * block : extent, part], projected[:extent, kpart],
                projected[:extent, vpart], c <= r,
            )
            heads_out[2 * i : 2 * i + 2, :, part] = out.reshape(2, crows, HEAD)

    heads_in[me_s] = heads_out[me_s]
    h_copies = []
    for d in order:
        dest = around(me_s, d, seq)
        h_copies.append(
            remote(
                heads_out.at[dest], heads_in.at[me_s], h_s.at[d - 1], h_r.at[d - 1],
                {"seq": dest},
            )
        )
    in_wout.wait()
    in_wup.wait()
    for copy in h_copies:
        copy.wait_recv()
    for j in range(seq):
        coarse_heads[:, j * own : (j + 1) * own] = heads_in[j]

    def partial(t, store):
        @pl.loop(0, fcols // tile)
        def _(i):
            cols = pl.ds(pl.multiple_of(i * tile, tile), tile)
            wcols = pl.ds(pl.multiple_of(t * fcols + i * tile, tile), tile)
            store(cols, dot32(coarse_heads[...], wout[:, wcols]))

    tp_order = sorted(range(1, tp), key=lambda d: abs(2 * d - tp))
    r1 = {}
    low_bits = tp_bits[::-1]
    for k, bit in enumerate(low_bits):
        for sub in range(tp - bit, 0, -2 * bit):
            dest = me_t
            for other in tp_bits:
                if sub & other:
                    dest = flip(dest, other)
            for low in low_bits[:k]:
                r1[sub + low].wait_recv()

            def put(cols, value, sub=sub, k=k):
                for low in low_bits[:k]:
                    value += recv1[sub + low - 1, :, cols].astype(jnp.float32)
                send1[sub - 1, :, cols] = value.astype(jnp.bfloat16)

            partial(dest, put)
            r1[sub] = remote(
                send1.at[sub - 1], recv1.at[sub - 1], r1_s.at[sub - 1], r1_r.at[sub - 1],
                {"tp": flip(me_t, bit)},
            )

    def keep(cols, value):
        short_cols[:, cols] = short_cols[:, cols].astype(jnp.bfloat16).astype(jnp.float32) + value

    partial(me_t, keep)
    for bit in low_bits:
        r1[bit].wait_recv()
    whole = short_cols[...]
    for bit in low_bits:
        whole += recv1[bit - 1].astype(jnp.float32)
    state[...] = whole.astype(jnp.bfloat16)
    slab = prior.shape[0]
    row_copy = remote(
        state.at[pl.ds(crows - slab, slab)], prior, row_s, row_r, {"seq": around(me_s, 1, seq)}
    )
    rolled = pltpu.roll(state[...].astype(jnp.float32), 1, 0)
    row_copy.wait_recv()
    previous = prior[...].astype(jnp.float32)[slab - 1 : slab, :]
    previous = jnp.where(me_s > 0, previous, 0.0)
    top = lax.broadcasted_iota(jnp.int32, rolled.shape, 0) == 0
    delayed = jnp.where(top, previous, rolled).astype(jnp.bfloat16)
    coarse_heads[...] = delayed

    @pl.loop(0, width // tile)
    def _(i):
        cols = pl.ds(pl.multiple_of(i * tile, tile), tile)
        short_cols[:, cols] = dot32(coarse_heads[...], wup[:, cols])

    r2 = []
    for d in tp_order:
        dest = around(me_t, d, tp)
        part = short_cols[pl.ds(pl.multiple_of(dest * pool_rows, pool_rows), pool_rows), :]
        send2[d - 1] = part.astype(jnp.bfloat16)
        r2.append(
            remote(
                send2.at[d - 1], recv2.at[d - 1], r2_s.at[d - 1], r2_r.at[d - 1], {"tp": dest}
            )
        )
    lifted = short_cols[pl.ds(pl.multiple_of(me_t * pool_rows, pool_rows), pool_rows), :]
    for copy in r2:
        copy.wait_recv()
    for d in range(1, tp):
        lifted += recv2[d - 1].astype(jnp.float32)
    spread = jnp.broadcast_to(lifted[:, None, :], (pool_rows, SHORT, width)).reshape(rows, width)
    result[...] = (fine_state[...].astype(jnp.float32) + spread).astype(jnp.bfloat16)
    w_flat = [copy for group in w_copies.values() for copy in group]
    for copy in w_flat + d_done + extra + done + h_copies + list(r1.values()) + [row_copy] + r2:
        copy.wait_send()


def head_body(
    tokens,
    fine_gain,
    fine_query,
    fine_keyval,
    fine_out,
    down_weight,
    coarse_gain,
    coarse_query,
    coarse_keyval,
    coarse_out,
    up_weight,
):
    seq, tp = lax.axis_size("seq"), lax.axis_size("tp")
    rows, width = tokens.shape
    depth, local_cols = coarse_query.shape
    own = local_cols // seq
    pool_rows = rows // SHORT
    crows = pool_rows * tp
    count = crows * seq
    bf, f32 = jnp.bfloat16, jnp.float32
    V = pltpu.VMEM
    dma = lambda n: pltpu.SemaphoreType.DMA((n,))
    one = pltpu.SemaphoreType.DMA
    anywhere = pl.BlockSpec(memory_space=pl.ANY)
    vmem = pl.BlockSpec(memory_space=pltpu.VMEM)
    return pl.pallas_call(
        functools.partial(section_kernel, seq, tp),
        out_shape=jax.ShapeDtypeStruct((rows, width), bf),
        in_specs=[anywhere, vmem, anywhere, anywhere, anywhere, anywhere, vmem, anywhere,
                  anywhere, anywhere, anywhere],
        out_specs=vmem,
        scratch_shapes=[
            V((2 * rows, width), bf), V(fine_query.shape, bf), V(fine_keyval.shape, bf),
            V(fine_out.shape, bf), V((tp,) + down_weight.shape, bf), V((seq, depth, 3 * own), bf),
            V(coarse_out.shape, bf), V(up_weight.shape, bf),
            V((2 * rows, width), bf), V((rows, width), bf), V((2 * rows, 2 * width), bf),
            V((rows, width), bf), V((rows, width), bf), V((seq * tp, pool_rows, width), bf),
            V((count, tp * local_cols), bf), V((count, 3 * own), bf), V((count, 3 * own), f32),
            V((seq, crows, own), bf), V((seq, crows, own), bf), V((crows, local_cols), bf),
            V((crows, local_cols), f32), V((tp - 1, crows, local_cols), bf),
            V((tp - 1, crows, local_cols), bf), V((crows, local_cols), bf), V((16, local_cols), bf),
            V((tp - 1, pool_rows, width), bf), V((tp - 1, pool_rows, width), bf),
            dma(11), one(()), one(()), dma(3 * (seq - 1)), dma(3 * (seq - 1)), dma(tp - 1), dma(tp - 1),
            dma(seq * tp - 1), dma(seq * tp - 1), dma(seq - 1), dma(seq - 1),
            dma(tp - 1), dma(tp - 1), one(()), one(()), dma(tp - 1), dma(tp - 1),
        ],
        compiler_params=pltpu.CompilerParams(
            collective_id=0, has_side_effects=True, vmem_limit_bytes=62 * 1024 * 1024
        ),
    )(tokens, fine_gain[None], fine_query, fine_keyval, fine_out, down_weight, coarse_gain[None],
      coarse_query, jnp.transpose(coarse_keyval, (1, 0, 2)), coarse_out, up_weight)


def chosen(*args):
    seq, tp = lax.axis_size("seq"), lax.axis_size("tp")
    local_heads = args[7].shape[1] // HEAD
    powers = seq & (seq - 1) == 0 and tp & (tp - 1) == 0 and seq > 1 and tp > 1
    square = args[10].shape[0] == args[10].shape[1] == args[7].shape[1]
    if local_heads % seq == 0 and args[0].shape[0] == WINDOW and powers and square:
        return head_body(*args)
    return body(*args)


def solution(mesh):
    return jax.shard_map(
        chosen,
        mesh=mesh,
        in_specs=(
            P(("seq", "tp"), None),
            P(),
            P(),
            P(),
            P(),
            P(None, "tp"),
            P(),
            P("seq", "tp"),
            P("seq", None, "tp"),
            P("tp", None),
            P("tp", None),
        ),
        out_specs=P(("seq", "tp"), None),
        check_vma=False,
    )
```
